256 devices in a mesh: groups: 2 (over y), dp: 16 (over z), tensor: 4 (over x), seq: 2 (over core).
Axes of the slice: x: 4, y: 2, z: 16, core: 2. Of those that a mesh axis runs over, the one named last changes fastest.
The devices are a block of a 4x16x16 slice.
Arguments:
- hidden: bfloat16 [1024, 64, 8192], P(('groups', 'dp', 'seq'), None, 'tensor'), parts along dimension 0, may hold values from -6 to 6
- lengths: int32 [1024], P(('groups', 'dp', 'seq')), parts along dimension 0, may hold values from 2 to 64
- answers: int32 [1024], P(('groups', 'dp', 'seq')), parts along dimension 0, may hold values from 0 to 63
- prompt_of: int32 [1024], P(('groups', 'dp', 'seq')), parts along dimension 0, may hold values from 0 to 31, as said below
- query_weight: bfloat16 [8192, 4096], P(('tensor', 'dp'))
- key_weight: bfloat16 [8192, 512], P('tensor')
- value_weight: bfloat16 [8192, 512], P('tensor'), may hold values from -0.0625 to 0.0625
- score_vec: float32 [4096], replicated, may hold values from -0.75 to 0.75
Outputs:
- vote_share: float32 [64, 64], P(('groups', 'dp')), parts along dimension 0
The draws below stay inside these ranges and needn't reach their ends.
There are 2 independent parts, one for each index of `groups`. The reference program is written for one: setup_inputs(seed, part) draws one part's arguments, and reference() takes and returns one part's arrays. A program takes and returns all parts, laid end to end along the dimension named above; an argument that names none is the same for every part. Nothing has to cross between parts.
Inputs may be any that keep to these rules, and one draw needn't show every extreme that they name: `prompt_of`: every prompt has exactly 16 samples. In every aligned block of 16 samples, exactly one sample belongs to each pair of prompts 2k and 2k + 1.
All inputs are finite; a program needn't handle non-finite values.
Results may differ from the reference program's by a relative error of at most 0.003.
Values may be sent and summed in bfloat16 or wider, within the bound.
No kernel may reach another device: no remote copies, remote signals or barrier semaphores. Data moves between devices by JAX's collectives and lax.ppermute only.
A program may use at most 64 MiB of HBM per device.

```python
import math
import jax
import jax.numpy as jnp
import numpy as np
from jax import lax

MODEL_WIDTH = 8192
HEAD_SIZE = 128
QUERY_HEADS = 32
KEY_VALUE_HEADS = 4
ANSWERS = 64
SAMPLES = 16
PROMPT_DEV = 2
SEQ_LEN = 64
SAMP_DEV = 32
DEV_SAMP = 16
PROMPTS = 32
SAMPLES_ALL = 512


def common_keys(key):
    offset_start = jax.random.normal(jax.random.fold_in(key, 3), (MODEL_WIDTH, KEY_VALUE_HEADS * HEAD_SIZE), jnp.float32)
    return jnp.clip(offset_start, -6.0, 6.0) / math.sqrt(MODEL_WIDTH)


def draw_key_weight(key, part):
    return common_keys(key).astype(jnp.bfloat16)


def draw_query_weight(key, part):
    noise = jnp.clip(jax.random.normal(jax.random.fold_in(key, 4), (MODEL_WIDTH, QUERY_HEADS * HEAD_SIZE), jnp.float32), -6.0, 6.0) / math.sqrt(MODEL_WIDTH)
    result = noise
    return result.astype(jnp.bfloat16)


def draw_prompt_of(key, part):
    group_total = SAMPLES_ALL // SAMP_DEV
    block_total = SAMPLES_ALL // DEV_SAMP
    per_piece = SAMP_DEV // block_total
    subkeys = jax.random.split(jax.random.fold_in(key, 7), group_total)
    orders = jax.vmap(lambda sub: jax.random.permutation(sub, SAMP_DEV))(subkeys)
    prompts = orders // SAMPLES + (jnp.arange(group_total, dtype=jnp.int32) * PROMPT_DEV)[:, None]
    layout = jnp.transpose(prompts.reshape(group_total, block_total, per_piece), (1, 0, 2)).reshape(block_total, DEV_SAMP)
    mixkeys = jax.random.split(jax.random.fold_in(key, 8), block_total)
    shuffled = jax.vmap(lambda sub, line: jax.random.permutation(sub, line))(mixkeys, layout)
    return shuffled.reshape(SAMPLES_ALL).astype(jnp.int32)


def set_ends(values, stream_key, smallest, largest):
    longest = values.shape.index(max(values.shape))
    spots = []
    for shift in (0, 1):
        where = [jax.random.randint(jax.random.fold_in(stream_key, axis), (), 0, length) for axis, length in enumerate(values.shape)]
        where[longest] = (where[longest] + shift) % values.shape[longest]
        spots.append(tuple(where))
    return values.at[spots[0]].set(smallest).at[spots[1]].set(largest)


def level_of(key, extent, shards, least, high):
    gain, own = 1.0, jax.random.fold_in(key, 6)
    for position, blocks in shards:
        heights = jnp.exp(jax.random.uniform(jax.random.fold_in(own, position), (blocks,), jnp.float32, least / len(shards), high / len(shards)))
        gain = gain * jnp.repeat(heights, extent[position] // blocks).reshape([-1 if axis == position else 1 for axis in range(len(extent))])
    return gain


def rank_table(number_of, skew):
    portions = [(1 << 20) // math.isqrt(rank ** skew) + 1 for rank in range(1, number_of + 1)]
    width = 1 + sum(portions) // (1 << 30)
    return np.cumsum(np.array([max(1, weight // width) for weight in portions]))


def skewed_ids(stream_key, extent, amount, slope):
    grid = rank_table(amount, slope)
    lot = jax.random.randint(jax.random.fold_in(stream_key, 1), extent, 0, int(grid[amount - 1]))
    standing = jnp.searchsorted(jnp.asarray(grid, jnp.int32), lot, side="right")
    return jax.random.permutation(jax.random.fold_in(stream_key, 2), amount)[standing].astype(jnp.int32)


def centred(key, dims, spread, bound, shards=(), held_as=jnp.bfloat16):
    factor_of = level_of(key, dims, shards, -0.22, 0.18) if shards else 1.0
    drawn = jax.random.normal(key, dims, jnp.float32) * spread * factor_of
    return jnp.minimum(jnp.maximum(drawn, -bound), bound).astype(held_as)


def setup_inputs(seed: int = 0, part: int = 0) -> dict:
    key_list = jax.random.split(jax.random.key(seed), 9)
    part_splits = jax.random.split(jax.random.fold_in(key_list[8], part), 9)
    return {
        "hidden": centred(part_splits[0], (SAMPLES_ALL, SEQ_LEN, MODEL_WIDTH), 1.0, 6.0, ((0, 32), (2, 4))),
        "lengths": set_ends(jax.random.randint(part_splits[1], (SAMPLES_ALL,), 2, SEQ_LEN + 1), jax.random.fold_in(part_splits[1], 1), 2, SEQ_LEN).astype(jnp.int32),
        "answers": set_ends(skewed_ids(part_splits[2], (SAMPLES_ALL,), ANSWERS, 2), jax.random.fold_in(part_splits[2], 3), 0, ANSWERS - 1).astype(jnp.int32),
        "prompt_of": draw_prompt_of(jax.random.fold_in(jax.random.fold_in(key_list[8], part), 71), part),
        "query_weight": draw_query_weight(jax.random.fold_in(key_list[8], 71), part),
        "key_weight": draw_key_weight(jax.random.fold_in(key_list[8], 71), part),
        "value_weight": centred(key_list[6], (MODEL_WIDTH, KEY_VALUE_HEADS * HEAD_SIZE), MODEL_WIDTH ** -0.5, 0.0625, ((0, 4),)),
        "score_vec": centred(key_list[7], (QUERY_HEADS * HEAD_SIZE,), (QUERY_HEADS * HEAD_SIZE // 64) ** -0.5, 0.75, (), jnp.float32),
    }


rope_base = 500000.0

def rotate(vectors, positions):
    halves = vectors.shape[-1] // 2
    frequency = rope_base ** (-jnp.arange(halves, dtype=jnp.float32) * 2.0 / vectors.shape[-1])
    angles = positions[..., None] * frequency
    cosine = jnp.cos(angles)
    sine_part = jnp.sin(angles)
    first_half = vectors[..., :halves]
    second_half = vectors[..., halves:]
    return jnp.concatenate([first_half * cosine - second_half * sine_part, second_half * cosine + first_half * sine_part], -1)

def reference(hidden, lengths, answers, prompt_of, query_weight, key_weight, value_weight, score_vec):
    sample_count, total_length, features = hidden.shape
    group_width = QUERY_HEADS // KEY_VALUE_HEADS
    key_positions = jnp.arange(total_length, dtype=jnp.float32)

    def score_block(inputs):
        block_rows, lengths_block = inputs
        block_number = block_rows.shape[0]
        flat_scores = block_rows.reshape(block_number * total_length, features)
        local_keys = jnp.dot(flat_scores, key_weight, preferred_element_type=jnp.float32).reshape(block_number, total_length, KEY_VALUE_HEADS, HEAD_SIZE)
        local_keys = rotate(local_keys, key_positions[None, :, None]).astype(jnp.bfloat16)
        local_values = jnp.dot(flat_scores, value_weight, preferred_element_type=jnp.float32).reshape(block_number, total_length, KEY_VALUE_HEADS, HEAD_SIZE).astype(jnp.bfloat16)
        last_pos = (lengths_block - 1).astype(jnp.int32)
        onehot = (jnp.arange(total_length, dtype=jnp.int32)[None, :] == last_pos[:, None]).astype(jnp.float32)
        final_row = jnp.einsum('bp,bpd->bd', onehot, block_rows.astype(jnp.float32)).astype(jnp.bfloat16)
        query_matrix = jnp.dot(final_row, query_weight, preferred_element_type=jnp.float32).reshape(block_number, KEY_VALUE_HEADS, group_width, HEAD_SIZE)
        query_matrix = rotate(query_matrix, last_pos.astype(jnp.float32)[:, None, None]).astype(jnp.bfloat16)
        scores = jnp.einsum('bgjd,bpgd->bgjp', query_matrix.astype(jnp.float32), local_keys.astype(jnp.float32)) / math.sqrt(HEAD_SIZE)
        visible = (jnp.arange(total_length, dtype=jnp.int32)[None, :] < lengths_block[:, None])[:, None, None, :]
        masked = jnp.where(visible, scores, -1e+30)
        row_maximum = lax.optimization_barrier(jnp.max(masked, axis=-1, keepdims=True))
        weights_soft = jnp.where(visible, jnp.exp(masked - row_maximum), 0.0)
        softmax_sum = lax.optimization_barrier(jnp.sum(weights_soft, axis=-1))
        weighted_values = jnp.einsum('bgjp,bpgd->bgjd', weights_soft, local_values.astype(jnp.float32), precision=lax.Precision.HIGHEST)
        attention = (weighted_values / softmax_sum[..., None]).astype(jnp.bfloat16).reshape(block_number, QUERY_HEADS * HEAD_SIZE)
        return jnp.dot(attention.astype(jnp.float32), score_vec, precision=lax.Precision.HIGHEST)
    blocks_total = sample_count // SAMPLES
    rating = lax.map(score_block, (hidden.reshape(blocks_total, SAMPLES, total_length, features), lengths.reshape(blocks_total, SAMPLES))).reshape(sample_count)
    reward = jax.nn.sigmoid(rating)
    onehot_prompt = (prompt_of[:, None] == jnp.arange(PROMPTS, dtype=jnp.int32)[None, :]).astype(jnp.float32)
    onehot_answer = (answers[:, None] == jnp.arange(ANSWERS, dtype=jnp.int32)[None, :]).astype(jnp.float32)
    tallies = jnp.dot(onehot_prompt.T, reward[:, None] * onehot_answer, precision=lax.Precision.HIGHEST)
    return tallies / lax.optimization_barrier(jnp.sum(tallies, axis=1, keepdims=True))
```

```python
import functools
import math

import jax
import jax.numpy as jnp
from jax import lax
from jax.experimental import pallas as pl
from jax.experimental.pallas import tpu as pltpu
from jax.sharding import PartitionSpec as P

HEAD_SIZE = 128
QUERY_HEADS = 32
KEY_VALUE_HEADS = 4
GROUP = QUERY_HEADS // KEY_VALUE_HEADS
ANSWERS = 64
PROMPT_DEV = 2
ROPE_BASE = 500000.0
BF = jnp.bfloat16
F32 = jnp.float32

VMEM = pl.BlockSpec(memory_space=pltpu.VMEM)
SMEM = pl.BlockSpec(memory_space=pltpu.SMEM)
ANY = pl.BlockSpec(memory_space=pl.ANY)


def cost(flops, bytes_accessed):
    return pl.CostEstimate(flops=flops, bytes_accessed=bytes_accessed, transcendentals=0)


def rope_tables(positions):
    halves = HEAD_SIZE // 2
    frequency = ROPE_BASE ** (-jnp.arange(halves, dtype=F32) * 2.0 / HEAD_SIZE)
    angles = positions[:, None] * frequency
    cosine, sine = jnp.cos(angles), jnp.sin(angles)
    return jnp.concatenate([cosine, cosine], -1), jnp.concatenate([-sine, sine], -1)


def rows_kernel(n_dp, lengths_ref, wide_ref, hidden_ref, out_ref, tiles, sems):
    samples, block = tiles.shape[0], tiles.shape[1]
    copies = []
    for i in range(samples):
        at = pl.multiple_of(((lengths_ref[i] - 1) // block) * block, block)
        copy = pltpu.make_async_copy(
            hidden_ref.at[i, pl.ds(at, block), :], tiles.at[i], sems.at[i]
        )
        copy.start()
        copies.append(copy)
    lane = lax.broadcasted_iota(jnp.int32, (samples, samples * block), 1)
    row = lax.broadcasted_iota(jnp.int32, (samples, samples * block), 0)
    inside = (wide_ref[:, : 1] - 1) % block
    pick = jnp.where(lane == row * block + inside, 1.0, 0.0).astype(BF)
    for copy in copies:
        copy.wait()
    stacked = tiles[...].reshape(samples * block, tiles.shape[2])
    rows = jnp.dot(pick, stacked, preferred_element_type=F32).astype(BF)
    width = rows.shape[1] // n_dp
    for d in range(n_dp):
        for side, source in enumerate((d, d ^ 1)):
            out_ref[d, :, side * width : (side + 1) * width] = rows[
                :, source * width : (source + 1) * width
            ]


def scoring_rows(lengths, wide, hidden, n_dp):
    samples, _, features = hidden.shape
    width = 2 * features // n_dp
    return pl.pallas_call(
        functools.partial(rows_kernel, n_dp),
        out_shape=jax.ShapeDtypeStruct((n_dp, samples, width), BF),
        in_specs=[SMEM, VMEM, ANY],
        out_specs=VMEM,
        scratch_shapes=[
            pltpu.VMEM((samples, 16, features), BF),
            pltpu.SemaphoreType.DMA((samples,)),
        ],
        cost_estimate=cost(2 * samples * 256 * features, samples * 16 * features * 2),
        name="scoring_rows",
    )(lengths, wide, hidden)


def cut_kernel(n_tensor, place_ref, weight_ref, *out_refs):
    t, parity = place_ref[0], place_ref[1]
    part = out_refs[0].shape[1]
    for side in range(2):
        for s in range(n_tensor):
            column = 2 * ((t + s) % n_tensor) + (parity ^ side)
            at = pl.multiple_of(column * part, part)
            out_refs[side * n_tensor + s][...] = weight_ref[:, pl.ds(at, part)]


def cut_weight(place, weight, n_tensor):
    rows, columns = weight.shape
    part = columns // (2 * n_tensor)
    count = 2 * n_tensor
    return pl.pallas_call(
        functools.partial(cut_kernel, n_tensor),
        out_shape=[jax.ShapeDtypeStruct((rows, part), BF)] * count,
        in_specs=[SMEM, VMEM],
        out_specs=[VMEM] * count,
        cost_estimate=cost(1000, 2 * rows * columns * 2),
        name="cut_weight",
    )(place, weight)


def kv_kernel(n_tensor, t_ref, x_ref, *refs):
    wk_refs = refs[:n_tensor]
    wv_ref, s_ref, cos_ref, sin_ref = refs[n_tensor : n_tensor + 4]
    out_refs = refs[n_tensor + 4 : 2 * n_tensor + 4]
    z_ref, w_ref = refs[2 * n_tensor + 4 :]
    step = pl.program_id(0)
    heads = QUERY_HEADS

    @pl.when(step == 0)
    def _():
        t = t_ref[0]
        head = lax.broadcasted_iota(jnp.int32, (heads, KEY_VALUE_HEADS * HEAD_SIZE), 0)
        column = lax.broadcasted_iota(jnp.int32, (heads, KEY_VALUE_HEADS * HEAD_SIZE), 1)
        spread = jnp.concatenate([s_ref[...]] * KEY_VALUE_HEADS, axis=1)
        full = jnp.where(head // GROUP == column // HEAD_SIZE, spread, 0.0)
        high = full.astype(BF)
        low = (full - high.astype(F32)).astype(BF)
        both = jnp.concatenate([high, low], axis=0)
        z = lax.dot_general(
            both, wv_ref[...], (((1,), (1,)), ((), ())), preferred_element_type=F32
        )
        z = z[:heads] + z[heads:]
        z_high = z.astype(BF)
        z_ref[:heads, :] = z_high
        z_ref[heads:, :] = (z - z_high.astype(F32)).astype(BF)
        for s in range(n_tensor):
            w_ref[:, s * HEAD_SIZE : (s + 1) * HEAD_SIZE] = wk_refs[s][...]

    x = x_ref[...]
    rows = x.shape[0]
    keys = jnp.dot(x, w_ref[...], preferred_element_type=F32)
    cosine = jnp.concatenate([cos_ref[...]] * (rows // cos_ref.shape[0]), axis=0)
    sine = jnp.concatenate([sin_ref[...]] * (rows // sin_ref.shape[0]), axis=0)
    at = pl.multiple_of(step * rows, rows)
    for s in range(n_tensor):
        k = keys[:, s * HEAD_SIZE : (s + 1) * HEAD_SIZE]
        rotated = k * cosine + pltpu.roll(k, HEAD_SIZE // 2, 1) * sine
        out_refs[s][pl.ds(at, rows), :] = rotated.astype(BF)
    u = lax.dot_general(
        z_ref[...], x, (((1,), (1,)), ((), ())), preferred_element_type=F32
    )
    u = u[:heads] + u[heads:]
    u_high = u.astype(BF)
    u_low = (u - u_high.astype(F32)).astype(BF)
    total = pl.num_programs(0) * rows
    for g in range(n_tensor):
        slot = (g - t_ref[0] + n_tensor) % n_tensor
        mine = jnp.concatenate(
            [u_high[g * GROUP : (g + 1) * GROUP], u_low[g * GROUP : (g + 1) * GROUP]], axis=0
        )
        for s in range(n_tensor):

            @pl.when(slot == s)
            def _():
                for c in range(rows // HEAD_SIZE):
                    base = total + (step * (rows // HEAD_SIZE) + c) * 2 * GROUP
                    out_refs[s][pl.ds(pl.multiple_of(base, 2 * GROUP), 2 * GROUP), :] = mine[
                        :, c * HEAD_SIZE : (c + 1) * HEAD_SIZE
                    ]


def keys_and_values(place, flat, key_weight, value_weight, score_rows, cosine, sine, n_tensor):
    total, features = flat.shape
    rows = 256
    packed = total + (total // HEAD_SIZE) * 2 * GROUP

    def whole(*dims):
        return pl.BlockSpec(dims, lambda i, p: (0,) * len(dims))

    def key_block(s):
        return pl.BlockSpec((features, HEAD_SIZE), lambda i, p: (0, (p[0] + s) % n_tensor))

    return pl.pallas_call(
        functools.partial(kv_kernel, n_tensor),
        grid_spec=pltpu.PrefetchScalarGridSpec(
            num_scalar_prefetch=1,
            grid=(total // rows,),
            in_specs=[pl.BlockSpec((rows, features), lambda i, p: (i, 0))]
            + [key_block(s) for s in range(n_tensor)]
            + [
                whole(*value_weight.shape),
                whole(*score_rows.shape),
                whole(*cosine.shape),
                whole(*sine.shape),
            ],
            out_specs=[whole(packed, HEAD_SIZE)] * n_tensor,
            scratch_shapes=[
                pltpu.VMEM((2 * QUERY_HEADS, features), BF),
                pltpu.VMEM((features, n_tensor * HEAD_SIZE), BF),
            ],
        ),
        out_shape=[jax.ShapeDtypeStruct((packed, HEAD_SIZE), BF)] * n_tensor,
        cost_estimate=cost(2 * total * features * 640, 9 * 2**20),
        name="keys_and_values",
    )(place, flat, *[key_weight] * n_tensor, value_weight, score_rows, cosine, sine)


def query_kernel(n_tensor, *refs):
    x_refs = refs[:n_tensor]
    w_refs = refs[n_tensor : 3 * n_tensor]
    out_ref = refs[3 * n_tensor]
    n_dp, heads, samples, _ = out_ref.shape
    x = jnp.concatenate(
        [x_refs[s][...].reshape(n_dp * samples, -1) for s in range(n_tensor)], axis=1
    )
    w = jnp.concatenate(
        [w_refs[side * n_tensor + s][...] for s in range(n_tensor) for side in range(2)], axis=0
    )
    q = jnp.dot(x, w, preferred_element_type=F32).astype(BF)
    for h in range(heads):
        out_ref[:, h, :, :] = q[:, h * HEAD_SIZE : (h + 1) * HEAD_SIZE].reshape(
            n_dp, samples, HEAD_SIZE
        )


def partial_queries(pieces, weights):
    n_dp, samples, width = pieces[0].shape
    heads = weights[0].shape[1] // HEAD_SIZE
    return pl.pallas_call(
        functools.partial(query_kernel, len(pieces)),
        out_shape=jax.ShapeDtypeStruct((n_dp, heads, samples, HEAD_SIZE), BF),
        in_specs=[VMEM] * (len(pieces) + len(weights)),
        out_specs=VMEM,
        cost_estimate=cost(2 * n_dp * samples * width * 4 * heads * HEAD_SIZE, 2 * 2**20),
        name="partial_queries",
    )(*pieces, *weights)


def attention_kernel(n_tensor, q_ref, *refs):
    kv_refs = refs[:n_tensor]
    wide_ref, cos_ref, sin_ref, prompt_ref, answer_ref, out_ref = refs[n_tensor:]
    n_dp, half, samples, _ = q_ref.shape
    q = jnp.zeros((2 * half * samples, HEAD_SIZE), F32)
    for pair in range(n_dp // 2):
        block = q_ref[2 * pair : 2 * pair + 2].reshape(2 * half * samples, HEAD_SIZE)
        q = q + block.astype(F32)
    heads = 2 * half
    cosine = jnp.concatenate([cos_ref[...]] * heads, axis=0)
    sine = jnp.concatenate([sin_ref[...]] * heads, axis=0)
    q = (q * cosine + pltpu.roll(q, HEAD_SIZE // 2, 1) * sine).astype(BF)
    total = samples * 64
    chunks = total // HEAD_SIZE
    lengths = jnp.concatenate([wide_ref[...]] * heads, axis=0)
    lane = lax.broadcasted_iota(jnp.int32, (heads * samples, HEAD_SIZE), 1)
    row = lax.broadcasted_iota(jnp.int32, (heads * samples, HEAD_SIZE), 0)
    start = (row % samples) * 64
    scores, values = [], []
    for c in range(chunks):
        k = kv_refs[0][c * HEAD_SIZE : (c + 1) * HEAD_SIZE].astype(F32)
        base = total + c * 2 * GROUP
        u = kv_refs[0][base : base + 2 * GROUP].astype(F32)
        for s in range(1, n_tensor):
            k = k + kv_refs[s][c * HEAD_SIZE : (c + 1) * HEAD_SIZE].astype(F32)
            u = u + kv_refs[s][base : base + 2 * GROUP].astype(F32)
        u = u[:GROUP] + u[GROUP:]
        score = lax.dot_general(
            q, k.astype(BF), (((1,), (1,)), ((), ())), preferred_element_type=F32
        ) / math.sqrt(HEAD_SIZE)
        position = lane + c * HEAD_SIZE - start
        scores.append(jnp.where((position >= 0) & (position < lengths), score, -1e30))
        values.append(
            jnp.broadcast_to(u[:, None, :], (heads, samples, HEAD_SIZE)).reshape(
                heads * samples, HEAD_SIZE
            )
        )
    top = scores[0]
    for c in range(1, chunks):
        top = jnp.maximum(top, scores[c])
    top = jnp.max(top, axis=1, keepdims=True)
    below = jnp.zeros_like(scores[0])
    above = jnp.zeros_like(scores[0])
    for c in range(chunks):
        weight = jnp.exp(scores[c] - top)
        below = below + weight
        above = above + weight * values[c]
    part = jnp.sum(above, axis=1, keepdims=True) / jnp.sum(below, axis=1, keepdims=True)
    rating = jnp.sum(part.reshape(heads, samples, 1), axis=0)
    out_rows = out_ref.shape[0]
    owner = lax.broadcasted_iota(jnp.int32, (out_rows, HEAD_SIZE), 0) // n_tensor
    column = lax.broadcasted_iota(jnp.int32, (out_rows, HEAD_SIZE), 1)
    out = jnp.zeros((out_rows, HEAD_SIZE), F32)
    for i in range(samples):
        prompt = prompt_ref[i]
        place = ((prompt % PROMPT_DEV) * ANSWERS + answer_ref[i]).astype(F32)
        value = jnp.broadcast_to(rating[i : i + 1, :], (out_rows, HEAD_SIZE))
        entry = jnp.where(column == 0, value, jnp.where(column == 1, place, 0.0))
        out = jnp.where(owner == prompt // PROMPT_DEV, entry, out)
    out_ref[...] = out


def partial_ratings(queries, kv, wide, cosine, sine, prompt_of, answers):
    n_tensor = len(kv)
    n_dp = queries.shape[0]
    return pl.pallas_call(
        functools.partial(attention_kernel, n_tensor),
        out_shape=jax.ShapeDtypeStruct((n_dp * n_tensor, HEAD_SIZE), F32),
        in_specs=[VMEM] * (n_tensor + 4) + [SMEM, SMEM],
        out_specs=VMEM,
        cost_estimate=cost(2 * 128 * 128 * 1024, 2 * 2**20),
        name="partial_ratings",
    )(queries, *kv, wide, cosine, sine, prompt_of, answers)


def tally_kernel(n_tensor, rows_ref, out_ref):
    rows = rows_ref[...]
    summed = rows.reshape(rows.shape[0] // n_tensor, n_tensor, HEAD_SIZE)
    rating = jnp.sum(summed[:, :, 0:1], axis=1)
    place = summed[:, 0, 1:2].astype(jnp.int32)
    reward = 1.0 / (1.0 + jnp.exp(-rating))
    lane = lax.broadcasted_iota(jnp.int32, (rating.shape[0], HEAD_SIZE), 1)
    out_ref[...] = jnp.sum(jnp.where(lane == place, reward, 0.0), axis=0, keepdims=True)


def half_tallies(rows, n_tensor):
    return pl.pallas_call(
        functools.partial(tally_kernel, n_tensor),
        out_shape=jax.ShapeDtypeStruct((1, HEAD_SIZE), F32),
        in_specs=[VMEM],
        out_specs=VMEM,
        name="half_tallies",
    )(rows)


def share_kernel(here_ref, there_ref, out_ref):
    total = here_ref[...] + there_ref[...]
    for q in range(PROMPT_DEV):
        tally = total[:, q * ANSWERS : (q + 1) * ANSWERS]
        out_ref[q : q + 1, :] = tally / jnp.sum(tally, axis=1, keepdims=True)


def shares(here, there):
    return pl.pallas_call(
        share_kernel,
        out_shape=jax.ShapeDtypeStruct((PROMPT_DEV, ANSWERS), F32),
        in_specs=[VMEM, VMEM],
        out_specs=VMEM,
        name="shares",
    )(here, there)


def shards(hidden, lengths, answers, prompt_of, query_weight, key_weight, value_weight, score_vec):
    samples, positions, features = hidden.shape
    n_dp, n_tensor, n_seq = (lax.axis_size(a) for a in ("dp", "tensor", "seq"))
    t = lax.axis_index("tensor").astype(jnp.int32)
    parity = lax.axis_index("dp").astype(jnp.int32) % 2
    place = jnp.stack([t, parity])
    wide = jnp.broadcast_to(lengths[:, None], (samples, HEAD_SIZE))

    def over_tensor(value, s):
        return lax.ppermute(value, "tensor", [(i, (i + s) % n_tensor) for i in range(n_tensor)])

    def weight_piece(value, side, s):
        if side == 0 and s == 0:
            return value
        pairs = [
            (d * n_tensor + i, (d ^ side) * n_tensor + (i + s) % n_tensor)
            for d in range(n_dp)
            for i in range(n_tensor)
        ]
        return lax.ppermute(value, ("dp", "tensor"), pairs)

    rows = scoring_rows(lengths, wide, hidden, n_dp)
    moved = lax.all_to_all(rows, "dp", 0, 0, tiled=True)

    cut = cut_weight(place, query_weight, n_tensor)
    weights = [weight_piece(cut[k], k // n_tensor, k % n_tensor) for k in range(2 * n_tensor)]

    key_cos, key_sin = rope_tables(jnp.arange(positions, dtype=F32))
    kv = keys_and_values(
        place,
        hidden.reshape(samples * positions, features),
        key_weight,
        value_weight,
        score_vec.reshape(QUERY_HEADS, HEAD_SIZE),
        key_cos,
        key_sin,
        n_tensor,
    )
    pieces = [moved] + [over_tensor(moved, s) for s in range(1, n_tensor)]
    queries = partial_queries(pieces, weights)
    arrived = lax.all_to_all(queries, "dp", 0, 0, tiled=True)
    kv = [kv[0]] + [over_tensor(kv[s], s) for s in range(1, n_tensor)]
    query_cos, query_sin = rope_tables((lengths - 1).astype(F32))
    rated = partial_ratings(arrived, kv, wide, query_cos, query_sin, prompt_of, answers)
    gathered = lax.all_to_all(rated, ("dp", "tensor"), 0, 0, tiled=True)
    here = half_tallies(gathered, n_tensor)
    there = lax.ppermute(here, "seq", [(i, (i + 1) % n_seq) for i in range(n_seq)])
    return shares(here, there)


def solution(mesh):
    placed = (
        P(("groups", "dp", "seq"), None, "tensor"),
        P(("groups", "dp", "seq")),
        P(("groups", "dp", "seq")),
        P(("groups", "dp", "seq")),
        P(("tensor", "dp"), None),
        P("tensor", None),
        P("tensor", None),
        P(),
    )
    return jax.shard_map(
        shards, mesh=mesh, in_specs=placed, out_specs=P(("groups", "dp"), None), check_vma=False
    )
```

```python
import functools
import math

import jax
import jax.numpy as jnp
from jax import lax
from jax.experimental import pallas as pl
from jax.experimental.pallas import tpu as pltpu
from jax.sharding import PartitionSpec as P

HEAD_SIZE = 128
QUERY_HEADS = 32
KEY_VALUE_HEADS = 4
GROUP = QUERY_HEADS // KEY_VALUE_HEADS
ANSWERS = 64
PROMPT_DEV = 2
ROPE_BASE = 500000.0
BF = jnp.bfloat16
F32 = jnp.float32

VMEM = pl.BlockSpec(memory_space=pltpu.VMEM)
SMEM = pl.BlockSpec(memory_space=pltpu.SMEM)
ANY = pl.BlockSpec(memory_space=pl.ANY)
HBM = pl.BlockSpec(memory_space=pltpu.HBM)


def limit(mib):
    return pltpu.CompilerParams(vmem_limit_bytes=mib * 2**20)


def cost(flops, bytes_accessed):
    return pl.CostEstimate(flops=flops, bytes_accessed=bytes_accessed, transcendentals=0)


def rope_tables(positions):
    halves = HEAD_SIZE // 2
    frequency = ROPE_BASE ** (-jnp.arange(halves, dtype=F32) * 2.0 / HEAD_SIZE)
    angles = positions[:, None] * frequency
    cosine, sine = jnp.cos(angles), jnp.sin(angles)
    return jnp.concatenate([cosine, cosine], -1), jnp.concatenate([-sine, sine], -1)


def rows_kernel(n_dp, lengths_ref, hidden_ref, out_ref, tiles, sems):
    samples, block = tiles.shape[0], tiles.shape[1]
    copies = []
    for i in range(samples):
        at = pl.multiple_of(((lengths_ref[i] - 1) // block) * block, block)
        copy = pltpu.make_async_copy(
            hidden_ref.at[i, pl.ds(at, block), :], tiles.at[i], sems.at[i]
        )
        copy.start()
        copies.append(copy)
    lane = lax.broadcasted_iota(jnp.int32, (samples, samples * block), 1)
    row = lax.broadcasted_iota(jnp.int32, (samples, samples * block), 0)
    chosen = jnp.zeros(lane.shape, jnp.int32)
    for i in range(samples):
        chosen = jnp.where(row == i, i * block + (lengths_ref[i] - 1) % block, chosen)
    pick = jnp.where(lane == chosen, 1.0, 0.0).astype(BF)
    for copy in copies:
        copy.wait()
    stacked = tiles[...].reshape(samples * block, tiles.shape[2])
    rows = jnp.dot(pick, stacked, preferred_element_type=F32).astype(BF)
    width = rows.shape[1] // n_dp
    for d in range(n_dp):
        for side, source in enumerate((d, d ^ 1)):
            out_ref[d, :, side * width : (side + 1) * width] = rows[
                :, source * width : (source + 1) * width
            ]


def scoring_rows(lengths, hidden, n_dp):
    samples, _, features = hidden.shape
    width = 2 * features // n_dp
    return pl.pallas_call(
        functools.partial(rows_kernel, n_dp),
        out_shape=jax.ShapeDtypeStruct((n_dp, samples, width), BF),
        in_specs=[SMEM, HBM],
        out_specs=VMEM,
        scratch_shapes=[
            pltpu.VMEM((samples, 16, features), BF),
            pltpu.SemaphoreType.DMA((samples,)),
        ],
        cost_estimate=cost(2 * samples * 256 * features, samples * 16 * features * 2),
        compiler_params=limit(62),
        name="scoring_rows",
    )(lengths, hidden)


def cut_kernel(n_tensor, weight_ref, *out_refs):
    t, parity = lax.axis_index("tensor"), lax.axis_index("dp") % 2
    part = out_refs[0].shape[1]
    for side in range(2):
        for s in range(n_tensor):
            column = 2 * ((t + s) % n_tensor) + (parity ^ side)
            at = pl.multiple_of(column * part, part)
            out_refs[side * n_tensor + s][...] = weight_ref[:, pl.ds(at, part)]


def cut_weight(weight, n_tensor):
    rows, columns = weight.shape
    part = columns // (2 * n_tensor)
    count = 2 * n_tensor
    return pl.pallas_call(
        functools.partial(cut_kernel, n_tensor),
        out_shape=[jax.ShapeDtypeStruct((rows, part), BF)] * count,
        in_specs=[VMEM],
        out_specs=[VMEM] * count,
        cost_estimate=cost(1000, 2 * rows * columns * 2),
        compiler_params=limit(4),
        name="cut_weight",
    )(weight)


def kv_kernel(
    n_tensor, h_ref, k_ref, v_ref, s_ref, cos_ref, sin_ref, after_ref, *refs
):
    out_refs = refs[:n_tensor]
    x_ref, wv_ref, w_ref, x_sems, w_sems = refs[n_tensor:]
    steps, rows, _ = x_ref.shape
    heads = QUERY_HEADS
    t = lax.axis_index("tensor")
    copies = [pltpu.make_async_copy(h_ref.at[pl.ds(0, rows), :], x_ref.at[0], x_sems.at[0])]
    for s in range(n_tensor):
        at = pl.multiple_of(((t + s) % n_tensor) * HEAD_SIZE, HEAD_SIZE)
        copies.append(
            pltpu.make_async_copy(
                k_ref.at[:, pl.ds(at, HEAD_SIZE)],
                w_ref.at[:, s * HEAD_SIZE : (s + 1) * HEAD_SIZE],
                w_sems.at[s],
            )
        )
    value_copy = pltpu.make_async_copy(v_ref, wv_ref, w_sems.at[n_tensor])
    copies.append(value_copy)
    for i in range(1, steps):
        copies.append(
            pltpu.make_async_copy(
                h_ref.at[pl.ds(i * rows, rows), :], x_ref.at[i], x_sems.at[i]
            )
        )
    for copy in copies:
        copy.start()

    head = lax.broadcasted_iota(jnp.int32, (heads, KEY_VALUE_HEADS * HEAD_SIZE), 0)
    column = lax.broadcasted_iota(jnp.int32, (heads, KEY_VALUE_HEADS * HEAD_SIZE), 1)
    spread = jnp.concatenate([s_ref[...]] * KEY_VALUE_HEADS, axis=1)
    full = jnp.where(head // GROUP == column // HEAD_SIZE, spread, 0.0)
    high = full.astype(BF)
    low = (full - high.astype(F32)).astype(BF)
    both = jnp.concatenate([high, low], axis=0)
    cosine = jnp.concatenate([cos_ref[...]] * (rows // cos_ref.shape[0]), axis=0)
    sine = jnp.concatenate([sin_ref[...]] * (rows // sin_ref.shape[0]), axis=0)

    for i in range(steps):
        copies[0 if i == 0 else n_tensor + 1 + i].wait()
        if i == 0:
            for s in range(n_tensor):
                copies[1 + s].wait()
        x = x_ref[i]
        keys = jnp.dot(x, w_ref[...], preferred_element_type=F32)
        for s in range(n_tensor):
            k = keys[:, s * HEAD_SIZE : (s + 1) * HEAD_SIZE]
            rotated = k * cosine + pltpu.roll(k, HEAD_SIZE // 2, 1) * sine
            out_refs[s][i * rows : (i + 1) * rows, :] = rotated.astype(BF)
        if i == 0:
            value_copy.wait()
            z = lax.dot_general(
                both, wv_ref[...], (((1,), (1,)), ((), ())), preferred_element_type=F32
            )
            z = z[:heads] + z[heads:]
            z_high = z.astype(BF)
            z_low = (z - z_high.astype(F32)).astype(BF)
            z = jnp.concatenate([z_high, z_low], axis=0)
        u = lax.dot_general(z, x, (((1,), (1,)), ((), ())), preferred_element_type=F32)
        u = u[:heads] + u[heads:]
        u_high = u.astype(BF)
        u_low = (u - u_high.astype(F32)).astype(BF)
        for g in range(n_tensor):
            slot = (g - t + n_tensor) % n_tensor
            mine = jnp.concatenate(
                [u_high[g * GROUP : (g + 1) * GROUP], u_low[g * GROUP : (g + 1) * GROUP]], axis=0
            )
            for s in range(n_tensor):

                @pl.when(slot == s)
                def _():
                    for c in range(rows // HEAD_SIZE):
                        base = steps * rows + (i * (rows // HEAD_SIZE) + c) * 2 * GROUP
                        out_refs[s][base : base + 2 * GROUP, :] = mine[
                            :, c * HEAD_SIZE : (c + 1) * HEAD_SIZE
                        ]


def keys_and_values(flat, key_weight, value_weight, score_rows, cosine, sine, after, n_tensor):
    total, features = flat.shape
    rows = 256
    packed = total + (total // HEAD_SIZE) * 2 * GROUP
    return pl.pallas_call(
        functools.partial(kv_kernel, n_tensor),
        in_specs=[HBM, HBM, HBM, VMEM, VMEM, VMEM, ANY],
        out_specs=[VMEM] * n_tensor,
        scratch_shapes=[
            pltpu.VMEM((total // rows, rows, features), BF),
            pltpu.VMEM(value_weight.shape, BF),
            pltpu.VMEM(key_weight.shape, BF),
            pltpu.SemaphoreType.DMA((total // rows,)),
            pltpu.SemaphoreType.DMA((n_tensor + 1,)),
        ],
        out_shape=[jax.ShapeDtypeStruct((packed, HEAD_SIZE), BF)] * n_tensor,
        cost_estimate=cost(2 * total * features * 640, 9 * 2**20),
        compiler_params=limit(52),
        name="keys_and_values",
    )(flat, key_weight, value_weight, score_rows, cosine, sine, after)


def query_kernel(n_tensor, *refs):
    x_refs = refs[:n_tensor]
    w_refs = refs[n_tensor : 3 * n_tensor]
    out_ref = refs[3 * n_tensor + 1]
    n_dp, heads, samples, _ = out_ref.shape
    x = jnp.concatenate(
        [x_refs[s][...].reshape(n_dp * samples, -1) for s in range(n_tensor)], axis=1
    )
    w = jnp.concatenate(
        [w_refs[side * n_tensor + s][...] for s in range(n_tensor) for side in range(2)], axis=0
    )
    q = jnp.dot(x, w, preferred_element_type=F32).astype(BF)
    for h in range(heads):
        out_ref[:, h, :, :] = q[:, h * HEAD_SIZE : (h + 1) * HEAD_SIZE].reshape(
            n_dp, samples, HEAD_SIZE
        )


def partial_queries(pieces, weights, after):
    n_dp, samples, width = pieces[0].shape
    heads = weights[0].shape[1] // HEAD_SIZE
    return pl.pallas_call(
        functools.partial(query_kernel, len(pieces)),
        out_shape=jax.ShapeDtypeStruct((n_dp, heads, samples, HEAD_SIZE), BF),
        in_specs=[VMEM] * (len(pieces) + len(weights)) + [ANY],
        out_specs=VMEM,
        cost_estimate=cost(2 * n_dp * samples * width * 4 * heads * HEAD_SIZE, 2 * 2**20),
        compiler_params=limit(8),
        name="partial_queries",
    )(*pieces, *weights, after)


def attention_kernel(n_tensor, q_ref, *refs):
    kv_refs = refs[:n_tensor]
    cos_ref, sin_ref, lengths_ref, prompt_ref, answer_ref, out_ref = refs[n_tensor:]
    n_dp, half, samples, _ = q_ref.shape
    q = jnp.zeros((2 * half * samples, HEAD_SIZE), F32)
    for pair in range(n_dp // 2):
        block = q_ref[2 * pair : 2 * pair + 2].reshape(2 * half * samples, HEAD_SIZE)
        q = q + block.astype(F32)
    heads = 2 * half
    cosine = jnp.concatenate([cos_ref[...]] * heads, axis=0)
    sine = jnp.concatenate([sin_ref[...]] * heads, axis=0)
    q = (q * cosine + pltpu.roll(q, HEAD_SIZE // 2, 1) * sine).astype(BF)
    total = samples * 64
    chunks = total // HEAD_SIZE
    own = lax.broadcasted_iota(jnp.int32, (samples, HEAD_SIZE), 0)
    lengths = jnp.zeros((samples, HEAD_SIZE), jnp.int32)
    for i in range(samples):
        lengths = jnp.where(own == i, lengths_ref[i], lengths)
    lengths = jnp.concatenate([lengths] * heads, axis=0)
    lane = lax.broadcasted_iota(jnp.int32, (heads * samples, HEAD_SIZE), 1)
    row = lax.broadcasted_iota(jnp.int32, (heads * samples, HEAD_SIZE), 0)
    start = (row % samples) * 64
    scores, values = [], []
    for c in range(chunks):
        k = kv_refs[0][c * HEAD_SIZE : (c + 1) * HEAD_SIZE].astype(F32)
        base = total + c * 2 * GROUP
        u = kv_refs[0][base : base + 2 * GROUP].astype(F32)
        for s in range(1, n_tensor):
            k = k + kv_refs[s][c * HEAD_SIZE : (c + 1) * HEAD_SIZE].astype(F32)
            u = u + kv_refs[s][base : base + 2 * GROUP].astype(F32)
        u = u[:GROUP] + u[GROUP:]
        score = lax.dot_general(
            q, k.astype(BF), (((1,), (1,)), ((), ())), preferred_element_type=F32
        ) / math.sqrt(HEAD_SIZE)
        position = lane + c * HEAD_SIZE - start
        scores.append(jnp.where((position >= 0) & (position < lengths), score, -1e30))
        values.append(
            jnp.broadcast_to(u[:, None, :], (heads, samples, HEAD_SIZE)).reshape(
                heads * samples, HEAD_SIZE
            )
        )
    top = scores[0]
    for c in range(1, chunks):
        top = jnp.maximum(top, scores[c])
    top = jnp.max(top, axis=1, keepdims=True)
    below = jnp.zeros_like(scores[0])
    above = jnp.zeros_like(scores[0])
    for c in range(chunks):
        weight = jnp.exp(scores[c] - top)
        below = below + weight
        above = above + weight * values[c]
    part = jnp.sum(above, axis=1, keepdims=True) / jnp.sum(below, axis=1, keepdims=True)
    rating = jnp.sum(part.reshape(heads, samples, 1), axis=0)
    out_rows = out_ref.shape[0]
    owner = lax.broadcasted_iota(jnp.int32, (out_rows, HEAD_SIZE), 0) // n_tensor
    column = lax.broadcasted_iota(jnp.int32, (out_rows, HEAD_SIZE), 1)
    out = jnp.zeros((out_rows, HEAD_SIZE), F32)
    for i in range(samples):
        prompt = prompt_ref[i]
        place = ((prompt % PROMPT_DEV) * ANSWERS + answer_ref[i]).astype(F32)
        value = jnp.broadcast_to(rating[i : i + 1, :], (out_rows, HEAD_SIZE))
        entry = jnp.where(column == 0, value, jnp.where(column == 1, place, 0.0))
        out = jnp.where(owner == prompt // PROMPT_DEV, entry, out)
    out_ref[...] = out


def partial_ratings(queries, kv, cosine, sine, lengths, prompt_of, answers):
    n_tensor = len(kv)
    n_dp = queries.shape[0]
    return pl.pallas_call(
        functools.partial(attention_kernel, n_tensor),
        out_shape=jax.ShapeDtypeStruct((n_dp * n_tensor, HEAD_SIZE), F32),
        in_specs=[VMEM] * (n_tensor + 3) + [SMEM] * 3,
        out_specs=VMEM,
        cost_estimate=cost(2 * 128 * 128 * 1024, 2 * 2**20),
        compiler_params=limit(12),
        name="partial_ratings",
    )(queries, *kv, cosine, sine, lengths, prompt_of, answers)


def tally_kernel(n_tensor, rows_ref, out_ref):
    rows = rows_ref[...]
    summed = rows.reshape(rows.shape[0] // n_tensor, n_tensor, HEAD_SIZE)
    rating = jnp.sum(summed[:, :, 0:1], axis=1)
    place = summed[:, 0, 1:2].astype(jnp.int32)
    reward = 1.0 / (1.0 + jnp.exp(-rating))
    lane = lax.broadcasted_iota(jnp.int32, (rating.shape[0], HEAD_SIZE), 1)
    out_ref[...] = jnp.sum(jnp.where(lane == place, reward, 0.0), axis=0, keepdims=True)


def half_tallies(rows, n_tensor):
    return pl.pallas_call(
        functools.partial(tally_kernel, n_tensor),
        out_shape=jax.ShapeDtypeStruct((1, HEAD_SIZE), F32),
        in_specs=[VMEM],
        out_specs=VMEM,
        compiler_params=limit(2),
        name="half_tallies",
    )(rows)


def share_kernel(here_ref, there_ref, out_ref):
    total = here_ref[...] + there_ref[...]
    for q in range(PROMPT_DEV):
        tally = total[:, q * ANSWERS : (q + 1) * ANSWERS]
        out_ref[q : q + 1, :] = tally / jnp.sum(tally, axis=1, keepdims=True)


def shares(here, there):
    return pl.pallas_call(
        share_kernel,
        out_shape=jax.ShapeDtypeStruct((PROMPT_DEV, ANSWERS), F32),
        in_specs=[VMEM, VMEM],
        out_specs=VMEM,
        compiler_params=limit(2),
        name="shares",
    )(here, there)


def shards(hidden, lengths, answers, prompt_of, query_weight, key_weight, value_weight, score_vec):
    samples, positions, features = hidden.shape
    n_dp, n_tensor, n_seq = (lax.axis_size(a) for a in ("dp", "tensor", "seq"))

    def over_tensor(value, s):
        return lax.ppermute(value, "tensor", [(i, (i + s) % n_tensor) for i in range(n_tensor)])

    def weight_piece(value, side, s):
        if side == 0 and s == 0:
            return value
        pairs = [
            (d * n_tensor + i, (d ^ side) * n_tensor + (i + s) % n_tensor)
            for d in range(n_dp)
            for i in range(n_tensor)
        ]
        return lax.ppermute(value, ("dp", "tensor"), pairs)

    rows = scoring_rows(lengths, hidden, n_dp)
    moved = lax.all_to_all(rows, "dp", 0, 0, tiled=True)

    cut = cut_weight(query_weight, n_tensor)
    weights = [weight_piece(cut[k], k // n_tensor, k % n_tensor) for k in range(2 * n_tensor)]

    key_cos, key_sin = rope_tables(jnp.arange(positions, dtype=F32))
    kv = keys_and_values(
        hidden.reshape(samples * positions, features),
        key_weight,
        value_weight,
        score_vec.reshape(QUERY_HEADS, HEAD_SIZE),
        key_cos,
        key_sin,
        moved,
        n_tensor,
    )
    pieces = [moved] + [over_tensor(moved, s) for s in range(1, n_tensor)]
    queries = partial_queries(pieces, weights, kv[0])
    queries, *kv = lax.optimization_barrier((queries, *kv))
    arrived = lax.all_to_all(queries, "dp", 0, 0, tiled=True)
    kv = [kv[0]] + [over_tensor(kv[s], s) for s in range(1, n_tensor)]
    query_cos, query_sin = rope_tables((lengths - 1).astype(F32))
    rated = partial_ratings(arrived, kv, query_cos, query_sin, lengths, prompt_of, answers)
    gathered = lax.all_to_all(rated, ("dp", "tensor"), 0, 0, tiled=True)
    here = half_tallies(gathered, n_tensor)
    there = lax.ppermute(here, "seq", [(i, (i + 1) % n_seq) for i in range(n_seq)])
    return shares(here, there)


def solution(mesh):
    placed = (
        P(("groups", "dp", "seq"), None, "tensor"),
        P(("groups", "dp", "seq")),
        P(("groups", "dp", "seq")),
        P(("groups", "dp", "seq")),
        P(("tensor", "dp"), None),
        P("tensor", None),
        P("tensor", None),
        P(),
    )
    return jax.shard_map(
        shards, mesh=mesh, in_specs=placed, out_specs=P(("groups", "dp"), None), check_vma=False
    )
```

```python
import functools
import math

import jax
import jax.numpy as jnp
from jax import lax
from jax.experimental import pallas as pl
from jax.experimental.pallas import tpu as pltpu
from jax.sharding import PartitionSpec as P


HEAD_SIZE = 128
QUERY_HEADS = 32
KEY_VALUE_HEADS = 4
GROUP = QUERY_HEADS // KEY_VALUE_HEADS
ANSWERS = 64
PROMPT_DEV = 2
ROPE_BASE = 500000.0
BF = jnp.bfloat16
F32 = jnp.float32

VMEM = pl.BlockSpec(memory_space=pltpu.VMEM)
SMEM = pl.BlockSpec(memory_space=pltpu.SMEM)
ANY = pl.BlockSpec(memory_space=pl.ANY)
HBM = pl.BlockSpec(memory_space=pltpu.HBM)


def limit(mib):
    return pltpu.CompilerParams(vmem_limit_bytes=mib * 2**20)


def cost(flops, bytes_accessed):
    return pl.CostEstimate(flops=flops, bytes_accessed=bytes_accessed, transcendentals=0)


def rope_tables(positions):
    halves = HEAD_SIZE // 2
    frequency = ROPE_BASE ** (-jnp.arange(halves, dtype=F32) * 2.0 / HEAD_SIZE)
    angles = positions[:, None] * frequency
    cosine, sine = jnp.cos(angles), jnp.sin(angles)
    return jnp.concatenate([cosine, cosine], -1), jnp.concatenate([-sine, sine], -1)


def rows_kernel(n_dp, lengths_ref, hidden_ref, out_ref, tiles, sems):
    samples, block = tiles.shape[0], tiles.shape[1]
    copies = []
    for i in range(samples):
        at = pl.multiple_of(((lengths_ref[i] - 1) // block) * block, block)
        copy = pltpu.make_async_copy(
            hidden_ref.at[i, pl.ds(at, block), :], tiles.at[i], sems.at[i]
        )
        copy.start()
        copies.append(copy)
    lane = lax.broadcasted_iota(jnp.int32, (samples, samples * block), 1)
    row = lax.broadcasted_iota(jnp.int32, (samples, samples * block), 0)
    chosen = jnp.zeros(lane.shape, jnp.int32)
    for i in range(samples):
        chosen = jnp.where(row == i, i * block + (lengths_ref[i] - 1) % block, chosen)
    pick = jnp.where(lane == chosen, 1.0, 0.0).astype(BF)
    for copy in copies:
        copy.wait()
    stacked = tiles[...].reshape(samples * block, tiles.shape[2])
    rows = jnp.dot(pick, stacked, preferred_element_type=F32).astype(BF)
    width = rows.shape[1] // n_dp
    for d in range(n_dp):
        for side, source in enumerate((d, d ^ 1)):
            out_ref[d, :, side * width : (side + 1) * width] = rows[
                :, source * width : (source + 1) * width
            ]


def scoring_rows(lengths, hidden, n_dp):
    samples, _, features = hidden.shape
    width = 2 * features // n_dp
    return pl.pallas_call(
        functools.partial(rows_kernel, n_dp),
        out_shape=jax.ShapeDtypeStruct((n_dp, samples, width), BF),
        in_specs=[SMEM, HBM],
        out_specs=VMEM,
        scratch_shapes=[
            pltpu.VMEM((samples, 16, features), BF),
            pltpu.SemaphoreType.DMA((samples,)),
        ],
        cost_estimate=cost(2 * samples * 256 * features, samples * 16 * features * 2),
        compiler_params=limit(62),
        name="scoring_rows",
    )(lengths, hidden)


def cut_kernel(n_tensor, weight_ref, *out_refs):
    t, side = lax.axis_index("tensor"), lax.axis_index("dp") % 2
    side = (side + lax.axis_index("seq")) % 2
    part = out_refs[0].shape[1]
    for s in range(n_tensor):
        at = pl.multiple_of((2 * ((t + s) % n_tensor) + side) * part, part)
        out_refs[s][...] = weight_ref[:, pl.ds(at, part)]


def cut_weight(weight, n_tensor):
    rows, columns = weight.shape
    part = columns // (2 * n_tensor)
    return pl.pallas_call(
        functools.partial(cut_kernel, n_tensor),
        out_shape=[jax.ShapeDtypeStruct((rows, part), BF)] * n_tensor,
        in_specs=[VMEM],
        out_specs=[VMEM] * n_tensor,
        cost_estimate=cost(1000, 2 * rows * columns * 2),
        compiler_params=limit(4),
        name="cut_weight",
    )(weight)


def stack_kernel(own_ref, *refs):
    out_ref = refs[-1]
    first = lax.axis_index("seq") == 0
    out_ref[0] = jnp.where(first, own_ref[...].astype(F32), refs[0][...].astype(F32)).astype(BF)
    for s in range(1, len(refs) - 1):
        out_ref[s] = refs[s][...]


def stacked_weight(own, arrived):
    return pl.pallas_call(
        stack_kernel,
        out_shape=jax.ShapeDtypeStruct((len(arrived), *own.shape), BF),
        in_specs=[VMEM] * (1 + len(arrived)),
        out_specs=VMEM,
        cost_estimate=cost(1000, 2**20),
        compiler_params=limit(4),
        name="stacked_weight",
    )(own, *arrived)


def kv_kernel(
    n_tensor, h_ref, k_ref, v_ref, s_ref, cos_ref, sin_ref, after_ref, *refs
):
    out_refs = refs[:n_tensor]
    x_ref, wv_ref, w_ref, x_sems, w_sems = refs[n_tensor:]
    steps, rows, _ = x_ref.shape
    heads = QUERY_HEADS
    t = lax.axis_index("tensor")
    copies = [pltpu.make_async_copy(h_ref.at[pl.ds(0, rows), :], x_ref.at[0], x_sems.at[0])]
    for s in range(n_tensor):
        at = pl.multiple_of(((t + s) % n_tensor) * HEAD_SIZE, HEAD_SIZE)
        copies.append(
            pltpu.make_async_copy(
                k_ref.at[:, pl.ds(at, HEAD_SIZE)],
                w_ref.at[:, s * HEAD_SIZE : (s + 1) * HEAD_SIZE],
                w_sems.at[s],
            )
        )
    value_copy = pltpu.make_async_copy(v_ref, wv_ref, w_sems.at[n_tensor])
    copies.append(value_copy)
    for i in range(1, steps):
        copies.append(
            pltpu.make_async_copy(
                h_ref.at[pl.ds(i * rows, rows), :], x_ref.at[i], x_sems.at[i]
            )
        )
    for copy in copies:
        copy.start()

    head = lax.broadcasted_iota(jnp.int32, (heads, KEY_VALUE_HEADS * HEAD_SIZE), 0)
    column = lax.broadcasted_iota(jnp.int32, (heads, KEY_VALUE_HEADS * HEAD_SIZE), 1)
    spread = jnp.concatenate([s_ref[...]] * KEY_VALUE_HEADS, axis=1)
    full = jnp.where(head // GROUP == column // HEAD_SIZE, spread, 0.0)
    high = full.astype(BF)
    low = (full - high.astype(F32)).astype(BF)
    both = jnp.concatenate([high, low], axis=0)
    cosine = jnp.concatenate([cos_ref[...]] * (rows // cos_ref.shape[0]), axis=0)
    sine = jnp.concatenate([sin_ref[...]] * (rows // sin_ref.shape[0]), axis=0)

    for i in range(steps):
        copies[0 if i == 0 else n_tensor + 1 + i].wait()
        if i == 0:
            for s in range(n_tensor):
                copies[1 + s].wait()
        x = x_ref[i]
        keys = jnp.dot(x, w_ref[...], preferred_element_type=F32)
        for s in range(n_tensor):
            k = keys[:, s * HEAD_SIZE : (s + 1) * HEAD_SIZE]
            rotated = k * cosine + pltpu.roll(k, HEAD_SIZE // 2, 1) * sine
            out_refs[s][i * rows : (i + 1) * rows, :] = rotated.astype(BF)
        if i == 0:
            value_copy.wait()
            z = lax.dot_general(
                both, wv_ref[...], (((1,), (1,)), ((), ())), preferred_element_type=F32
            )
            z = z[:heads] + z[heads:]
            z_high = z.astype(BF)
            z_low = (z - z_high.astype(F32)).astype(BF)
            z = jnp.concatenate([z_high, z_low], axis=0)
        u = lax.dot_general(z, x, (((1,), (1,)), ((), ())), preferred_element_type=F32)
        u = u[:heads] + u[heads:]
        u_high = u.astype(BF)
        u_low = (u - u_high.astype(F32)).astype(BF)
        for g in range(n_tensor):
            slot = (g - t + n_tensor) % n_tensor
            mine = jnp.concatenate(
                [u_high[g * GROUP : (g + 1) * GROUP], u_low[g * GROUP : (g + 1) * GROUP]], axis=0
            )
            for s in range(n_tensor):

                @pl.when(slot == s)
                def _():
                    for c in range(rows // HEAD_SIZE):
                        base = steps * rows + (i * (rows // HEAD_SIZE) + c) * 2 * GROUP
                        out_refs[s][base : base + 2 * GROUP, :] = mine[
                            :, c * HEAD_SIZE : (c + 1) * HEAD_SIZE
                        ]


def keys_and_values(flat, key_weight, value_weight, score_rows, cosine, sine, after, n_tensor):
    total, features = flat.shape
    rows = 256
    packed = total + (total // HEAD_SIZE) * 2 * GROUP
    return pl.pallas_call(
        functools.partial(kv_kernel, n_tensor),
        in_specs=[HBM, HBM, HBM, VMEM, VMEM, VMEM, ANY],
        out_specs=[VMEM] * n_tensor,
        scratch_shapes=[
            pltpu.VMEM((total // rows, rows, features), BF),
            pltpu.VMEM(value_weight.shape, BF),
            pltpu.VMEM(key_weight.shape, BF),
            pltpu.SemaphoreType.DMA((total // rows,)),
            pltpu.SemaphoreType.DMA((n_tensor + 1,)),
        ],
        out_shape=[jax.ShapeDtypeStruct((packed, HEAD_SIZE), BF)] * n_tensor,
        cost_estimate=cost(2 * total * features * 640, 9 * 2**20),
        compiler_params=limit(52),
        name="keys_and_values",
    )(flat, key_weight, value_weight, score_rows, cosine, sine, after)


def query_kernel(n_tensor, *refs):
    x_refs = refs[:n_tensor]
    here_ref, there_ref, _, out_ref = refs[n_tensor:]
    n_dp, heads, samples, _ = out_ref.shape
    depth = here_ref.shape[1]
    seq = lax.axis_index("seq")
    columns, weights = [], []
    for s in range(n_tensor):
        for side, w_ref in ((seq, here_ref), (1 - seq, there_ref)):
            at = pl.multiple_of(side * depth, depth)
            columns.append(x_refs[s][:, :, pl.ds(at, depth)].reshape(n_dp * samples, depth))
            weights.append(w_ref[s])
    x = jnp.concatenate(columns, axis=1)
    w = jnp.concatenate(weights, axis=0)
    q = jnp.dot(x, w, preferred_element_type=F32).astype(BF)
    for h in range(heads):
        out_ref[:, h, :, :] = q[:, h * HEAD_SIZE : (h + 1) * HEAD_SIZE].reshape(
            n_dp, samples, HEAD_SIZE
        )


def partial_queries(pieces, here, there, after):
    n_dp, samples, width = pieces[0].shape
    heads = here.shape[2] // HEAD_SIZE
    return pl.pallas_call(
        functools.partial(query_kernel, len(pieces)),
        out_shape=jax.ShapeDtypeStruct((n_dp, heads, samples, HEAD_SIZE), BF),
        in_specs=[VMEM] * (len(pieces) + 2) + [ANY],
        out_specs=VMEM,
        cost_estimate=cost(2 * n_dp * samples * width * 4 * heads * HEAD_SIZE, 2 * 2**20),
        compiler_params=limit(8),
        name="partial_queries",
    )(*pieces, here, there, after)


def attention_kernel(n_tensor, copies, q_ref, *refs):
    kv_refs = refs[:n_tensor]
    cos_ref, sin_ref, lengths_ref, prompt_ref, answer_ref, out_ref = refs[n_tensor:]
    n_dp, half, samples, _ = q_ref.shape
    q = jnp.zeros((2 * half * samples, HEAD_SIZE), F32)
    for pair in range(n_dp // 2):
        block = q_ref[2 * pair : 2 * pair + 2].reshape(2 * half * samples, HEAD_SIZE)
        q = q + block.astype(F32)
    heads = 2 * half
    cosine = jnp.concatenate([cos_ref[...]] * heads, axis=0)
    sine = jnp.concatenate([sin_ref[...]] * heads, axis=0)
    q = (q * cosine + pltpu.roll(q, HEAD_SIZE // 2, 1) * sine).astype(BF)
    total = samples * 64
    chunks = total // HEAD_SIZE
    own = lax.broadcasted_iota(jnp.int32, (samples, HEAD_SIZE), 0)
    lengths = jnp.zeros((samples, HEAD_SIZE), jnp.int32)
    for i in range(samples):
        lengths = jnp.where(own == i, lengths_ref[i], lengths)
    lengths = jnp.concatenate([lengths] * heads, axis=0)
    lane = lax.broadcasted_iota(jnp.int32, (heads * samples, HEAD_SIZE), 1)
    row = lax.broadcasted_iota(jnp.int32, (heads * samples, HEAD_SIZE), 0)
    start = (row % samples) * 64
    scores, values = [], []
    for c in range(chunks):
        k = kv_refs[0][c * HEAD_SIZE : (c + 1) * HEAD_SIZE].astype(F32)
        base = total + c * 2 * GROUP
        u = kv_refs[0][base : base + 2 * GROUP].astype(F32)
        for s in range(1, n_tensor):
            k = k + kv_refs[s][c * HEAD_SIZE : (c + 1) * HEAD_SIZE].astype(F32)
            u = u + kv_refs[s][base : base + 2 * GROUP].astype(F32)
        u = u[:GROUP] + u[GROUP:]
        score = lax.dot_general(
            q, k.astype(BF), (((1,), (1,)), ((), ())), preferred_element_type=F32
        ) / math.sqrt(HEAD_SIZE)
        position = lane + c * HEAD_SIZE - start
        scores.append(jnp.where((position >= 0) & (position < lengths), score, -1e30))
        values.append(
            jnp.broadcast_to(u[:, None, :], (heads, samples, HEAD_SIZE)).reshape(
                heads * samples, HEAD_SIZE
            )
        )
    top = scores[0]
    for c in range(1, chunks):
        top = jnp.maximum(top, scores[c])
    top = jnp.max(top, axis=1, keepdims=True)
    below = jnp.zeros_like(scores[0])
    above = jnp.zeros_like(scores[0])
    for c in range(chunks):
        weight = jnp.exp(scores[c] - top)
        below = below + weight
        above = above + weight * values[c]
    part = jnp.sum(above, axis=1, keepdims=True) / jnp.sum(below, axis=1, keepdims=True)
    rating = jnp.sum(part.reshape(heads, samples, 1), axis=0)
    out_rows = out_ref.shape[0]
    owner = lax.broadcasted_iota(jnp.int32, (out_rows, HEAD_SIZE), 0) // copies
    column = lax.broadcasted_iota(jnp.int32, (out_rows, HEAD_SIZE), 1)
    out = jnp.zeros((out_rows, HEAD_SIZE), F32)
    for i in range(samples):
        prompt = prompt_ref[i]
        place = ((prompt % PROMPT_DEV) * ANSWERS + answer_ref[i]).astype(F32)
        value = jnp.broadcast_to(rating[i : i + 1, :], (out_rows, HEAD_SIZE))
        entry = jnp.where(column == 0, value, jnp.where(column == 1, place, 0.0))
        out = jnp.where(owner == prompt // PROMPT_DEV, entry, out)
    out_ref[...] = out


def partial_ratings(queries, kv, cosine, sine, lengths, prompt_of, answers, copies):
    n_tensor = len(kv)
    n_dp = queries.shape[0]
    return pl.pallas_call(
        functools.partial(attention_kernel, n_tensor, copies),
        out_shape=jax.ShapeDtypeStruct((n_dp * copies, HEAD_SIZE), F32),
        in_specs=[VMEM] * (n_tensor + 3) + [SMEM] * 3,
        out_specs=VMEM,
        cost_estimate=cost(2 * 128 * 128 * 1024, 2 * 2**20),
        compiler_params=limit(12),
        name="partial_ratings",
    )(queries, *kv, cosine, sine, lengths, prompt_of, answers)


def share_kernel(n_tensor, rows_ref, out_ref):
    rows = rows_ref[...].reshape(-1, n_tensor, 2, HEAD_SIZE)
    total = jnp.zeros((1, HEAD_SIZE), F32)
    for seq in range(2):
        rating = rows[:, 0, seq, 0:1]
        for s in range(1, n_tensor):
            rating = rating + rows[:, s, seq, 0:1]
        place = rows[:, 0, seq, 1:2].astype(jnp.int32)
        reward = 1.0 / (1.0 + jnp.exp(-rating))
        lane = lax.broadcasted_iota(jnp.int32, (rating.shape[0], HEAD_SIZE), 1)
        total = total + jnp.sum(jnp.where(lane == place, reward, 0.0), axis=0, keepdims=True)
    for q in range(PROMPT_DEV):
        tally = total[:, q * ANSWERS : (q + 1) * ANSWERS]
        out_ref[q : q + 1, :] = tally / jnp.sum(tally, axis=1, keepdims=True)


def shares(rows, n_tensor):
    return pl.pallas_call(
        functools.partial(share_kernel, n_tensor),
        out_shape=jax.ShapeDtypeStruct((PROMPT_DEV, ANSWERS), F32),
        in_specs=[VMEM],
        out_specs=VMEM,
        compiler_params=limit(2),
        name="shares",
    )(rows)


def shards(hidden, lengths, answers, prompt_of, query_weight, key_weight, value_weight, score_vec):
    samples, positions, features = hidden.shape
    n_dp, n_tensor, n_seq = (lax.axis_size(a) for a in ("dp", "tensor", "seq"))

    def over_tensor(value, s):
        return lax.ppermute(value, "tensor", [(i, (i + s) % n_tensor) for i in range(n_tensor)])

    def weight_piece(value, s):
        pairs = [
            (
                (d * n_tensor + i) * n_seq + c,
                ((d ^ c) * n_tensor + (i + s) % n_tensor) * n_seq + c,
            )
            for d in range(n_dp)
            for i in range(n_tensor)
            for c in range(n_seq)
            if s or c
        ]
        return lax.ppermute(value, ("dp", "tensor", "seq"), pairs)

    rows = scoring_rows(lengths, hidden, n_dp)
    moved = lax.all_to_all(rows, "dp", 0, 0, tiled=True)

    cut = cut_weight(query_weight, n_tensor)
    arrived_weight = [weight_piece(cut[s], s) for s in range(n_tensor)]

    key_cos, key_sin = rope_tables(jnp.arange(positions, dtype=F32))
    kv = keys_and_values(
        hidden.reshape(samples * positions, features),
        key_weight,
        value_weight,
        score_vec.reshape(QUERY_HEADS, HEAD_SIZE),
        key_cos,
        key_sin,
        cut[0],
        n_tensor,
    )
    moved, *kv = lax.optimization_barrier((moved, *kv))
    pieces = [moved] + [over_tensor(moved, s) for s in range(1, n_tensor)]
    here = stacked_weight(cut[0], arrived_weight)
    there = lax.ppermute(here, "seq", [(i, (i + 1) % n_seq) for i in range(n_seq)])
    queries = partial_queries(pieces, here, there, kv[0])
    kv = [kv[0]] + [over_tensor(kv[s], s) for s in range(1, n_tensor)]
    arrived = lax.all_to_all(queries, "dp", 0, 0, tiled=True)
    query_cos, query_sin = rope_tables((lengths - 1).astype(F32))
    rated = partial_ratings(
        arrived, kv, query_cos, query_sin, lengths, prompt_of, answers, n_tensor * n_seq
    )
    gathered = lax.all_to_all(rated, ("dp", "tensor", "seq"), 0, 0, tiled=True)
    return shares(gathered, n_tensor)


def solution(mesh):
    placed = (
        P(("groups", "dp", "seq"), None, "tensor"),
        P(("groups", "dp", "seq")),
        P(("groups", "dp", "seq")),
        P(("groups", "dp", "seq")),
        P(("tensor", "dp"), None),
        P("tensor", None),
        P("tensor", None),
        P(),
    )

    return jax.shard_map(
        shards, mesh=mesh, in_specs=placed, out_specs=P(("groups", "dp"), None), check_vma=False
    )
```

```python
import functools
import math

import jax
import jax.numpy as jnp
from jax import lax
from jax.experimental import pallas as pl
from jax.experimental.pallas import tpu as pltpu
from jax.sharding import PartitionSpec as P


HEAD_SIZE = 128
QUERY_HEADS = 32
KEY_VALUE_HEADS = 4
GROUP = QUERY_HEADS // KEY_VALUE_HEADS
ANSWERS = 64
PROMPT_DEV = 2
ROPE_BASE = 500000.0
BF = jnp.bfloat16
F32 = jnp.float32

VMEM = pl.BlockSpec(memory_space=pltpu.VMEM)
SMEM = pl.BlockSpec(memory_space=pltpu.SMEM)
ANY = pl.BlockSpec(memory_space=pl.ANY)
HBM = pl.BlockSpec(memory_space=pltpu.HBM)


def limit(mib):
    return pltpu.CompilerParams(vmem_limit_bytes=mib * 2**20)


def cost(flops, bytes_accessed):
    return pl.CostEstimate(flops=flops, bytes_accessed=bytes_accessed, transcendentals=0)


def rope_tables(positions):
    halves = HEAD_SIZE // 2
    frequency = ROPE_BASE ** (-jnp.arange(halves, dtype=F32) * 2.0 / HEAD_SIZE)
    angles = positions[:, None] * frequency
    cosine, sine = jnp.cos(angles), jnp.sin(angles)
    return jnp.concatenate([cosine, cosine], -1), jnp.concatenate([-sine, sine], -1)


def rows_kernel(n_dp, lengths_ref, hidden_ref, out_ref, tiles, sems):
    samples, block = tiles.shape[0], tiles.shape[1]
    copies = []
    for i in range(samples):
        at = pl.multiple_of(((lengths_ref[i] - 1) // block) * block, block)
        copy = pltpu.make_async_copy(
            hidden_ref.at[i, pl.ds(at, block), :], tiles.at[i], sems.at[i]
        )
        copy.start()
        copies.append(copy)
    lane = lax.broadcasted_iota(jnp.int32, (samples, samples * block), 1)
    row = lax.broadcasted_iota(jnp.int32, (samples, samples * block), 0)
    chosen = jnp.zeros(lane.shape, jnp.int32)
    for i in range(samples):
        chosen = jnp.where(row == i, i * block + (lengths_ref[i] - 1) % block, chosen)
    pick = jnp.where(lane == chosen, 1.0, 0.0).astype(BF)
    for copy in copies:
        copy.wait()
    stacked = tiles[...].reshape(samples * block, tiles.shape[2])
    rows = jnp.dot(pick, stacked, preferred_element_type=F32).astype(BF)
    width = rows.shape[1] // n_dp
    for d in range(n_dp):
        for side, source in enumerate((d, d ^ 1)):
            out_ref[d, :, side * width : (side + 1) * width] = rows[
                :, source * width : (source + 1) * width
            ]


def scoring_rows(lengths, hidden, n_dp):
    samples, _, features = hidden.shape
    width = 2 * features // n_dp
    return pl.pallas_call(
        functools.partial(rows_kernel, n_dp),
        out_shape=jax.ShapeDtypeStruct((n_dp, samples, width), BF),
        in_specs=[SMEM, HBM],
        out_specs=VMEM,
        scratch_shapes=[
            pltpu.VMEM((samples, 16, features), BF),
            pltpu.SemaphoreType.DMA((samples,)),
        ],
        cost_estimate=cost(2 * samples * 256 * features, samples * 16 * features * 2),
        compiler_params=limit(62),
        name="scoring_rows",
    )(lengths, hidden)


def cut_kernel(n_tensor, weight_ref, *out_refs):
    t, side = lax.axis_index("tensor"), lax.axis_index("dp") % 2
    side = (side + lax.axis_index("seq")) % 2
    part = out_refs[0].shape[1]
    for s in range(n_tensor):
        at = pl.multiple_of((2 * ((t + s) % n_tensor) + side) * part, part)
        out_refs[s][...] = weight_ref[:, pl.ds(at, part)]


def cut_weight(weight, n_tensor):
    rows, columns = weight.shape
    part = columns // (2 * n_tensor)
    return pl.pallas_call(
        functools.partial(cut_kernel, n_tensor),
        out_shape=[jax.ShapeDtypeStruct((rows, part), BF)] * n_tensor,
        in_specs=[VMEM],
        out_specs=[VMEM] * n_tensor,
        cost_estimate=cost(1000, 2 * rows * columns * 2),
        compiler_params=limit(4),
        name="cut_weight",
    )(weight)


def stack_kernel(own_ref, *refs):
    out_ref = refs[-1]
    first = lax.axis_index("seq") == 0
    out_ref[0] = jnp.where(first, own_ref[...].astype(F32), refs[0][...].astype(F32)).astype(BF)
    for s in range(1, len(refs) - 1):
        out_ref[s] = refs[s][...]


def stacked_weight(own, arrived):
    return pl.pallas_call(
        stack_kernel,
        out_shape=jax.ShapeDtypeStruct((len(arrived), *own.shape), BF),
        in_specs=[VMEM] * (1 + len(arrived)),
        out_specs=VMEM,
        cost_estimate=cost(1000, 2**20),
        compiler_params=limit(4),
        name="stacked_weight",
    )(own, *arrived)


def kv_kernel(
    n_tensor, h_ref, k_ref, v_ref, s_ref, cos_ref, sin_ref, after_ref, *refs
):
    out_refs = refs[:n_tensor]
    x_ref, wv_ref, w_ref, x_sems, w_sems = refs[n_tensor:]
    steps, rows, _ = x_ref.shape
    heads = QUERY_HEADS
    t = lax.axis_index("tensor")
    copies = [pltpu.make_async_copy(h_ref.at[pl.ds(0, rows), :], x_ref.at[0], x_sems.at[0])]
    for s in range(n_tensor):
        at = pl.multiple_of(((t + s) % n_tensor) * HEAD_SIZE, HEAD_SIZE)
        copies.append(
            pltpu.make_async_copy(
                k_ref.at[:, pl.ds(at, HEAD_SIZE)],
                w_ref.at[:, s * HEAD_SIZE : (s + 1) * HEAD_SIZE],
                w_sems.at[s],
            )
        )
    value_copy = pltpu.make_async_copy(v_ref, wv_ref, w_sems.at[n_tensor])
    copies.append(value_copy)
    for i in range(1, steps):
        copies.append(
            pltpu.make_async_copy(
                h_ref.at[pl.ds(i * rows, rows), :], x_ref.at[i], x_sems.at[i]
            )
        )
    for copy in copies:
        copy.start()

    head = lax.broadcasted_iota(jnp.int32, (heads, KEY_VALUE_HEADS * HEAD_SIZE), 0)
    column = lax.broadcasted_iota(jnp.int32, (heads, KEY_VALUE_HEADS * HEAD_SIZE), 1)
    spread = jnp.concatenate([s_ref[...]] * KEY_VALUE_HEADS, axis=1)
    full = jnp.where(head // GROUP == column // HEAD_SIZE, spread, 0.0)
    high = full.astype(BF)
    low = (full - high.astype(F32)).astype(BF)
    both = jnp.concatenate([high, low], axis=0)
    cosine = jnp.concatenate([cos_ref[...]] * (rows // cos_ref.shape[0]), axis=0)
    sine = jnp.concatenate([sin_ref[...]] * (rows // sin_ref.shape[0]), axis=0)

    for i in range(steps):
        copies[0 if i == 0 else n_tensor + 1 + i].wait()
        if i == 0:
            for s in range(n_tensor):
                copies[1 + s].wait()
        x = x_ref[i]
        keys = jnp.dot(x, w_ref[...], preferred_element_type=F32)
        for s in range(n_tensor):
            k = keys[:, s * HEAD_SIZE : (s + 1) * HEAD_SIZE]
            rotated = k * cosine + pltpu.roll(k, HEAD_SIZE // 2, 1) * sine
            out_refs[s][i * rows : (i + 1) * rows, :] = rotated.astype(BF)
        if i == 0:
            value_copy.wait()
            z = lax.dot_general(
                both, wv_ref[...], (((1,), (1,)), ((), ())), preferred_element_type=F32
            )
            z = z[:heads] + z[heads:]
            z_high = z.astype(BF)
            z_low = (z - z_high.astype(F32)).astype(BF)
            z = jnp.concatenate([z_high, z_low], axis=0)
        u = lax.dot_general(z, x, (((1,), (1,)), ((), ())), preferred_element_type=F32)
        u = u[:heads] + u[heads:]
        u_high = u.astype(BF)
        u_low = (u - u_high.astype(F32)).astype(BF)
        for g in range(n_tensor):
            slot = (g - t + n_tensor) % n_tensor
            mine = jnp.concatenate(
                [u_high[g * GROUP : (g + 1) * GROUP], u_low[g * GROUP : (g + 1) * GROUP]], axis=0
            )
            for s in range(n_tensor):

                @pl.when(slot == s)
                def _():
                    for c in range(rows // HEAD_SIZE):
                        base = steps * rows + (i * (rows // HEAD_SIZE) + c) * 2 * GROUP
                        out_refs[s][base : base + 2 * GROUP, :] = mine[
                            :, c * HEAD_SIZE : (c + 1) * HEAD_SIZE
                        ]


def keys_and_values(flat, key_weight, value_weight, score_rows, cosine, sine, after, n_tensor):
    total, features = flat.shape
    rows = 256
    packed = total + (total // HEAD_SIZE) * 2 * GROUP
    return pl.pallas_call(
        functools.partial(kv_kernel, n_tensor),
        in_specs=[HBM, HBM, HBM, VMEM, VMEM, VMEM, ANY],
        out_specs=[VMEM] * n_tensor,
        scratch_shapes=[
            pltpu.VMEM((total // rows, rows, features), BF),
            pltpu.VMEM(value_weight.shape, BF),
            pltpu.VMEM(key_weight.shape, BF),
            pltpu.SemaphoreType.DMA((total // rows,)),
            pltpu.SemaphoreType.DMA((n_tensor + 1,)),
        ],
        out_shape=[jax.ShapeDtypeStruct((packed, HEAD_SIZE), BF)] * n_tensor,
        cost_estimate=cost(2 * total * features * 640, 9 * 2**20),
        compiler_params=limit(52),
        name="keys_and_values",
    )(flat, key_weight, value_weight, score_rows, cosine, sine, after)


def query_kernel(n_tensor, *refs):
    x_refs = refs[:n_tensor]
    here_ref, there_ref, _, out_ref = refs[n_tensor:]
    n_dp, heads, samples, _ = out_ref.shape
    depth = here_ref.shape[1]
    seq = lax.axis_index("seq")
    columns, weights = [], []
    for s in range(n_tensor):
        for side, w_ref in ((seq, here_ref), (1 - seq, there_ref)):
            at = pl.multiple_of(side * depth, depth)
            columns.append(x_refs[s][:, :, pl.ds(at, depth)].reshape(n_dp * samples, depth))
            weights.append(w_ref[s])
    x = jnp.concatenate(columns, axis=1)
    w = jnp.concatenate(weights, axis=0)
    q = jnp.dot(x, w, preferred_element_type=F32).astype(BF)
    for h in range(heads):
        out_ref[:, h, :, :] = q[:, h * HEAD_SIZE : (h + 1) * HEAD_SIZE].reshape(
            n_dp, samples, HEAD_SIZE
        )


def partial_queries(pieces, here, there, after):
    n_dp, samples, width = pieces[0].shape
    heads = here.shape[2] // HEAD_SIZE
    return pl.pallas_call(
        functools.partial(query_kernel, len(pieces)),
        out_shape=jax.ShapeDtypeStruct((n_dp, heads, samples, HEAD_SIZE), BF),
        in_specs=[VMEM] * (len(pieces) + 2) + [ANY],
        out_specs=VMEM,
        cost_estimate=cost(2 * n_dp * samples * width * 4 * heads * HEAD_SIZE, 2 * 2**20),
        compiler_params=limit(8),
        name="partial_queries",
    )(*pieces, here, there, after)


def sum_kernel(q_ref, cos_ref, sin_ref, out_ref):
    n_dp, half, samples, _ = q_ref.shape
    heads = 2 * half
    q = jnp.zeros((heads * samples, HEAD_SIZE), F32)
    for pair in range(n_dp // 2):
        block = q_ref[2 * pair : 2 * pair + 2].reshape(heads * samples, HEAD_SIZE)
        q = q + block.astype(F32)
    cosine = jnp.concatenate([cos_ref[...]] * heads, axis=0)
    sine = jnp.concatenate([sin_ref[...]] * heads, axis=0)
    out_ref[...] = (q * cosine + pltpu.roll(q, HEAD_SIZE // 2, 1) * sine).astype(BF)


def summed_queries(arrived, cosine, sine):
    _, half, samples, _ = arrived.shape
    return pl.pallas_call(
        sum_kernel,
        out_shape=jax.ShapeDtypeStruct((2 * half * samples, HEAD_SIZE), BF),
        in_specs=[VMEM] * 3,
        out_specs=VMEM,
        compiler_params=limit(4),
        name="summed_queries",
    )(arrived, cosine, sine)


def attention_kernel(n_tensor, copies, q_ref, *refs):
    kv_refs = refs[:n_tensor]
    lengths_ref, prompt_ref, answer_ref, out_ref = refs[n_tensor:]
    samples = lengths_ref.shape[0]
    heads = q_ref.shape[0] // samples
    q = q_ref[...]
    total = samples * 64
    chunks = total // HEAD_SIZE
    own = lax.broadcasted_iota(jnp.int32, (samples, HEAD_SIZE), 0)
    lengths = jnp.zeros((samples, HEAD_SIZE), jnp.int32)
    for i in range(samples):
        lengths = jnp.where(own == i, lengths_ref[i], lengths)
    lengths = jnp.concatenate([lengths] * heads, axis=0)
    lane = lax.broadcasted_iota(jnp.int32, (heads * samples, HEAD_SIZE), 1)
    row = lax.broadcasted_iota(jnp.int32, (heads * samples, HEAD_SIZE), 0)
    start = (row % samples) * 64
    scores, values = [], []
    for c in range(chunks):
        k = kv_refs[0][c * HEAD_SIZE : (c + 1) * HEAD_SIZE].astype(F32)
        base = total + c * 2 * GROUP
        u = kv_refs[0][base : base + 2 * GROUP].astype(F32)
        for s in range(1, n_tensor):
            k = k + kv_refs[s][c * HEAD_SIZE : (c + 1) * HEAD_SIZE].astype(F32)
            u = u + kv_refs[s][base : base + 2 * GROUP].astype(F32)
        u = u[:GROUP] + u[GROUP:]
        score = lax.dot_general(
            q, k.astype(BF), (((1,), (1,)), ((), ())), preferred_element_type=F32
        ) / math.sqrt(HEAD_SIZE)
        position = lane + c * HEAD_SIZE - start
        scores.append(jnp.where((position >= 0) & (position < lengths), score, -1e30))
        values.append(
            jnp.broadcast_to(u[:, None, :], (heads, samples, HEAD_SIZE)).reshape(
                heads * samples, HEAD_SIZE
            )
        )
    top = scores[0]
    for c in range(1, chunks):
        top = jnp.maximum(top, scores[c])
    top = jnp.max(top, axis=1, keepdims=True)
    below = jnp.zeros_like(scores[0])
    above = jnp.zeros_like(scores[0])
    for c in range(chunks):
        weight = jnp.exp(scores[c] - top)
        below = below + weight
        above = above + weight * values[c]
    part = jnp.sum(above, axis=1, keepdims=True) / jnp.sum(below, axis=1, keepdims=True)
    rating = jnp.sum(part.reshape(heads, samples, 1), axis=0)
    out_rows = out_ref.shape[0]
    owner = lax.broadcasted_iota(jnp.int32, (out_rows, HEAD_SIZE), 0) // copies
    column = lax.broadcasted_iota(jnp.int32, (out_rows, HEAD_SIZE), 1)
    out = jnp.zeros((out_rows, HEAD_SIZE), F32)
    for i in range(samples):
        prompt = prompt_ref[i]
        place = ((prompt % PROMPT_DEV) * ANSWERS + answer_ref[i]).astype(F32)
        value = jnp.broadcast_to(rating[i : i + 1, :], (out_rows, HEAD_SIZE))
        entry = jnp.where(column == 0, value, jnp.where(column == 1, place, 0.0))
        out = jnp.where(owner == prompt // PROMPT_DEV, entry, out)
    out_ref[...] = out


def partial_ratings(queries, kv, lengths, prompt_of, answers, n_dp, copies):
    n_tensor = len(kv)
    return pl.pallas_call(
        functools.partial(attention_kernel, n_tensor, copies),
        out_shape=jax.ShapeDtypeStruct((n_dp * copies, HEAD_SIZE), F32),
        in_specs=[VMEM] * (n_tensor + 1) + [SMEM] * 3,
        out_specs=VMEM,
        cost_estimate=cost(2 * 128 * 128 * 1024, 2 * 2**20),
        compiler_params=limit(12),
        name="partial_ratings",
    )(queries, *kv, lengths, prompt_of, answers)


def share_kernel(n_tensor, rows_ref, out_ref):
    rows = rows_ref[...].reshape(-1, n_tensor, 2, HEAD_SIZE)
    total = jnp.zeros((1, HEAD_SIZE), F32)
    for seq in range(2):
        rating = rows[:, 0, seq, 0:1]
        for s in range(1, n_tensor):
            rating = rating + rows[:, s, seq, 0:1]
        place = rows[:, 0, seq, 1:2].astype(jnp.int32)
        reward = 1.0 / (1.0 + jnp.exp(-rating))
        lane = lax.broadcasted_iota(jnp.int32, (rating.shape[0], HEAD_SIZE), 1)
        total = total + jnp.sum(jnp.where(lane == place, reward, 0.0), axis=0, keepdims=True)
    for q in range(PROMPT_DEV):
        tally = total[:, q * ANSWERS : (q + 1) * ANSWERS]
        out_ref[q : q + 1, :] = tally / jnp.sum(tally, axis=1, keepdims=True)


def shares(rows, n_tensor):
    return pl.pallas_call(
        functools.partial(share_kernel, n_tensor),
        out_shape=jax.ShapeDtypeStruct((PROMPT_DEV, ANSWERS), F32),
        in_specs=[VMEM],
        out_specs=VMEM,
        compiler_params=limit(2),
        name="shares",
    )(rows)


def shards(hidden, lengths, answers, prompt_of, query_weight, key_weight, value_weight, score_vec):
    samples, positions, features = hidden.shape
    n_dp, n_tensor, n_seq = (lax.axis_size(a) for a in ("dp", "tensor", "seq"))

    def over_tensor(value, s):
        return lax.ppermute(value, "tensor", [(i, (i + s) % n_tensor) for i in range(n_tensor)])

    def weight_piece(value, s):
        pairs = [
            (
                (d * n_tensor + i) * n_seq + c,
                ((d ^ c) * n_tensor + (i + s) % n_tensor) * n_seq + c,
            )
            for d in range(n_dp)
            for i in range(n_tensor)
            for c in range(n_seq)
            if s or c
        ]
        return lax.ppermute(value, ("dp", "tensor", "seq"), pairs)

    rows = scoring_rows(lengths, hidden, n_dp)
    moved = lax.all_to_all(rows, "dp", 0, 0, tiled=True)

    cut = cut_weight(query_weight, n_tensor)
    arrived_weight = [weight_piece(cut[s], s) for s in range(n_tensor)]

    key_cos, key_sin = rope_tables(jnp.arange(positions, dtype=F32))
    kv = keys_and_values(
        hidden.reshape(samples * positions, features),
        key_weight,
        value_weight,
        score_vec.reshape(QUERY_HEADS, HEAD_SIZE),
        key_cos,
        key_sin,
        cut[0],
        n_tensor,
    )
    moved, *kv = lax.optimization_barrier((moved, *kv))
    pieces = [moved] + [over_tensor(moved, s) for s in range(1, n_tensor)]
    here = stacked_weight(cut[0], arrived_weight)
    there = lax.ppermute(here, "seq", [(i, (i + 1) % n_seq) for i in range(n_seq)])
    queries = partial_queries(pieces, here, there, kv[0])
    query_cos, query_sin = rope_tables((lengths - 1).astype(F32))
    queries, query_cos, query_sin = lax.optimization_barrier((queries, query_cos, query_sin))
    kv = [kv[0]] + [over_tensor(kv[s], s) for s in range(1, n_tensor)]
    arrived = lax.all_to_all(queries, "dp", 0, 0, tiled=True)
    summed = summed_queries(arrived, query_cos, query_sin)
    rated = partial_ratings(summed, kv, lengths, prompt_of, answers, n_dp, n_tensor * n_seq)
    gathered = lax.all_to_all(rated, ("dp", "tensor", "seq"), 0, 0, tiled=True)
    return shares(gathered, n_tensor)


def solution(mesh):
    placed = (
        P(("groups", "dp", "seq"), None, "tensor"),
        P(("groups", "dp", "seq")),
        P(("groups", "dp", "seq")),
        P(("groups", "dp", "seq")),
        P(("tensor", "dp"), None),
        P("tensor", None),
        P("tensor", None),
        P(),
    )

    return jax.shard_map(
        shards, mesh=mesh, in_specs=placed, out_specs=P(("groups", "dp"), None), check_vma=False
    )
```

```python
import functools
import math

import jax
import jax.numpy as jnp
from jax import lax
from jax.experimental import pallas as pl
from jax.experimental.pallas import tpu as pltpu
from jax.sharding import PartitionSpec as P


HEAD_SIZE = 128
QUERY_HEADS = 32
KEY_VALUE_HEADS = 4
GROUP = QUERY_HEADS // KEY_VALUE_HEADS
ANSWERS = 64
PROMPT_DEV = 2
ROPE_BASE = 500000.0
BF = jnp.bfloat16
F32 = jnp.float32

VMEM = pl.BlockSpec(memory_space=pltpu.VMEM)
SMEM = pl.BlockSpec(memory_space=pltpu.SMEM)
ANY = pl.BlockSpec(memory_space=pl.ANY)
HBM = pl.BlockSpec(memory_space=pltpu.HBM)


def limit(mib):
    return pltpu.CompilerParams(vmem_limit_bytes=mib * 2**20)


def cost(flops, bytes_accessed):
    return pl.CostEstimate(flops=flops, bytes_accessed=bytes_accessed, transcendentals=0)


def rope_tables(positions):
    halves = HEAD_SIZE // 2
    frequency = ROPE_BASE ** (-jnp.arange(halves, dtype=F32) * 2.0 / HEAD_SIZE)
    angles = positions[:, None] * frequency
    cosine, sine = jnp.cos(angles), jnp.sin(angles)
    return jnp.concatenate([cosine, cosine], -1), jnp.concatenate([-sine, sine], -1)


def rows_kernel(n_dp, lengths_ref, hidden_ref, out_ref, tiles, sems):
    samples, block = tiles.shape[0], tiles.shape[1]
    copies = []
    for i in range(samples):
        at = pl.multiple_of(((lengths_ref[i] - 1) // block) * block, block)
        copy = pltpu.make_async_copy(
            hidden_ref.at[i, pl.ds(at, block), :], tiles.at[i], sems.at[i]
        )
        copy.start()
        copies.append(copy)
    lane = lax.broadcasted_iota(jnp.int32, (samples, samples * block), 1)
    row = lax.broadcasted_iota(jnp.int32, (samples, samples * block), 0)
    chosen = jnp.zeros(lane.shape, jnp.int32)
    for i in range(samples):
        chosen = jnp.where(row == i, i * block + (lengths_ref[i] - 1) % block, chosen)
    pick = jnp.where(lane == chosen, 1.0, 0.0).astype(BF)
    for copy in copies:
        copy.wait()
    stacked = tiles[...].reshape(samples * block, tiles.shape[2])
    rows = jnp.dot(pick, stacked, preferred_element_type=F32).astype(BF)
    width = rows.shape[1] // n_dp
    for d in range(n_dp):
        for side, source in enumerate((d, d ^ 1)):
            out_ref[d, :, side * width : (side + 1) * width] = rows[
                :, source * width : (source + 1) * width
            ]


def scoring_rows(lengths, hidden, n_dp):
    samples, _, features = hidden.shape
    width = 2 * features // n_dp
    return pl.pallas_call(
        functools.partial(rows_kernel, n_dp),
        out_shape=jax.ShapeDtypeStruct((n_dp, samples, width), BF),
        in_specs=[SMEM, HBM],
        out_specs=VMEM,
        scratch_shapes=[
            pltpu.VMEM((samples, 8, features), BF),
            pltpu.SemaphoreType.DMA((samples,)),
        ],
        cost_estimate=cost(2 * samples * 256 * features, samples * 16 * features * 2),
        compiler_params=limit(62),
        name="scoring_rows",
    )(lengths, hidden)


def cut_kernel(n_tensor, weight_ref, *out_refs):
    t, side = lax.axis_index("tensor"), lax.axis_index("dp") % 2
    side = (side + lax.axis_index("seq")) % 2
    part = out_refs[0].shape[1]
    for s in range(n_tensor):
        at = pl.multiple_of((2 * ((t + s) % n_tensor) + side) * part, part)
        out_refs[s][...] = weight_ref[:, pl.ds(at, part)]


def cut_weight(weight, n_tensor):
    rows, columns = weight.shape
    part = columns // (2 * n_tensor)
    return pl.pallas_call(
        functools.partial(cut_kernel, n_tensor),
        out_shape=[jax.ShapeDtypeStruct((rows, part), BF)] * n_tensor,
        in_specs=[VMEM],
        out_specs=[VMEM] * n_tensor,
        cost_estimate=cost(1000, 2 * rows * columns * 2),
        compiler_params=limit(4),
        name="cut_weight",
    )(weight)


def stack_kernel(own_ref, *refs):
    out_ref = refs[-1]
    first = lax.axis_index("seq") == 0
    out_ref[0] = jnp.where(first, own_ref[...].astype(F32), refs[0][...].astype(F32)).astype(BF)
    for s in range(1, len(refs) - 1):
        out_ref[s] = refs[s][...]


def stacked_weight(own, arrived):
    return pl.pallas_call(
        stack_kernel,
        out_shape=jax.ShapeDtypeStruct((len(arrived), *own.shape), BF),
        in_specs=[VMEM] * (1 + len(arrived)),
        out_specs=VMEM,
        cost_estimate=cost(1000, 2**20),
        compiler_params=limit(4),
        name="stacked_weight",
    )(own, *arrived)


def kv_kernel(
    n_tensor, h_ref, k_ref, v_ref, s_ref, cos_ref, sin_ref, after_ref, *refs
):
    out_refs = refs[:n_tensor]
    x_ref, wv_ref, w_ref, x_sems, w_sems = refs[n_tensor:]
    steps, rows, _ = x_ref.shape
    heads = QUERY_HEADS
    t = lax.axis_index("tensor")
    copies = [pltpu.make_async_copy(h_ref.at[pl.ds(0, rows), :], x_ref.at[0], x_sems.at[0])]
    for s in range(n_tensor):
        at = pl.multiple_of(((t + s) % n_tensor) * HEAD_SIZE, HEAD_SIZE)
        copies.append(
            pltpu.make_async_copy(
                k_ref.at[:, pl.ds(at, HEAD_SIZE)],
                w_ref.at[:, s * HEAD_SIZE : (s + 1) * HEAD_SIZE],
                w_sems.at[s],
            )
        )
    value_copy = pltpu.make_async_copy(v_ref, wv_ref, w_sems.at[n_tensor])
    copies.append(value_copy)
    for i in range(1, steps):
        copies.append(
            pltpu.make_async_copy(
                h_ref.at[pl.ds(i * rows, rows), :], x_ref.at[i], x_sems.at[i]
            )
        )
    first = 1 + n_tensor
    for copy in copies[:first]:
        copy.start()

    head = lax.broadcasted_iota(jnp.int32, (heads, KEY_VALUE_HEADS * HEAD_SIZE), 0)
    column = lax.broadcasted_iota(jnp.int32, (heads, KEY_VALUE_HEADS * HEAD_SIZE), 1)
    spread = jnp.concatenate([s_ref[...]] * KEY_VALUE_HEADS, axis=1)
    full = jnp.where(head // GROUP == column // HEAD_SIZE, spread, 0.0)
    high = full.astype(BF)
    low = (full - high.astype(F32)).astype(BF)
    both = jnp.concatenate([high, low], axis=0)
    cosine = jnp.concatenate([cos_ref[...]] * (rows // cos_ref.shape[0]), axis=0)
    sine = jnp.concatenate([sin_ref[...]] * (rows // sin_ref.shape[0]), axis=0)

    for i in range(steps):
        copies[0 if i == 0 else first + i].wait()
        if i == 0:
            value_copy.start()
            for s in range(n_tensor):
                copies[1 + s].wait()
            copies[first + 1].start()
            copies[first + 2].start()
        x = x_ref[i]
        keys = jnp.dot(x, w_ref[...], preferred_element_type=F32)
        for s in range(n_tensor):
            k = keys[:, s * HEAD_SIZE : (s + 1) * HEAD_SIZE]
            rotated = k * cosine + pltpu.roll(k, HEAD_SIZE // 2, 1) * sine
            out_refs[s][i * rows : (i + 1) * rows, :] = rotated.astype(BF)
        if i == 0:
            value_copy.wait()
            for copy in copies[first + 3 :]:
                copy.start()
            z = lax.dot_general(
                both, wv_ref[...], (((1,), (1,)), ((), ())), preferred_element_type=F32
            )
            z = z[:heads] + z[heads:]
            z_high = z.astype(BF)
            z_low = (z - z_high.astype(F32)).astype(BF)
            z = jnp.concatenate([z_high, z_low], axis=0)
        u = lax.dot_general(z, x, (((1,), (1,)), ((), ())), preferred_element_type=F32)
        u = u[:heads] + u[heads:]
        u_high = u.astype(BF)
        u_low = (u - u_high.astype(F32)).astype(BF)
        for g in range(n_tensor):
            slot = (g - t + n_tensor) % n_tensor
            mine = jnp.concatenate(
                [u_high[g * GROUP : (g + 1) * GROUP], u_low[g * GROUP : (g + 1) * GROUP]], axis=0
            )
            for s in range(n_tensor):

                @pl.when(slot == s)
                def _():
                    for c in range(rows // HEAD_SIZE):
                        base = steps * rows + (i * (rows // HEAD_SIZE) + c) * 2 * GROUP
                        out_refs[s][base : base + 2 * GROUP, :] = mine[
                            :, c * HEAD_SIZE : (c + 1) * HEAD_SIZE
                        ]


def keys_and_values(flat, key_weight, value_weight, score_rows, cosine, sine, after, n_tensor):
    total, features = flat.shape
    rows = 256
    packed = total + (total // HEAD_SIZE) * 2 * GROUP
    return pl.pallas_call(
        functools.partial(kv_kernel, n_tensor),
        in_specs=[HBM, HBM, HBM, VMEM, VMEM, VMEM, ANY],
        out_specs=[VMEM] * n_tensor,
        scratch_shapes=[
            pltpu.VMEM((total // rows, rows, features), BF),
            pltpu.VMEM(value_weight.shape, BF),
            pltpu.VMEM(key_weight.shape, BF),
            pltpu.SemaphoreType.DMA((total // rows,)),
            pltpu.SemaphoreType.DMA((n_tensor + 1,)),
        ],
        out_shape=[jax.ShapeDtypeStruct((packed, HEAD_SIZE), BF)] * n_tensor,
        cost_estimate=cost(2 * total * features * 640, 9 * 2**20),
        compiler_params=limit(52),
        name="keys_and_values",
    )(flat, key_weight, value_weight, score_rows, cosine, sine, after)


def query_kernel(n_tensor, *refs):
    x_refs = refs[:n_tensor]
    here_ref, there_ref, _, out_ref = refs[n_tensor:]
    n_dp, heads, samples, _ = out_ref.shape
    depth = here_ref.shape[1]
    seq = lax.axis_index("seq")
    columns, weights = [], []
    for s in range(n_tensor):
        for side, w_ref in ((seq, here_ref), (1 - seq, there_ref)):
            at = pl.multiple_of(side * depth, depth)
            columns.append(x_refs[s][:, :, pl.ds(at, depth)].reshape(n_dp * samples, depth))
            weights.append(w_ref[s])
    x = jnp.concatenate(columns, axis=1)
    w = jnp.concatenate(weights, axis=0)
    q = jnp.dot(x, w, preferred_element_type=F32).astype(BF)
    for h in range(heads):
        out_ref[:, h, :, :] = q[:, h * HEAD_SIZE : (h + 1) * HEAD_SIZE].reshape(
            n_dp, samples, HEAD_SIZE
        )


def partial_queries(pieces, here, there, after):
    n_dp, samples, width = pieces[0].shape
    heads = here.shape[2] // HEAD_SIZE
    return pl.pallas_call(
        functools.partial(query_kernel, len(pieces)),
        out_shape=jax.ShapeDtypeStruct((n_dp, heads, samples, HEAD_SIZE), BF),
        in_specs=[VMEM] * (len(pieces) + 2) + [ANY],
        out_specs=VMEM,
        cost_estimate=cost(2 * n_dp * samples * width * 4 * heads * HEAD_SIZE, 2 * 2**20),
        compiler_params=limit(8),
        name="partial_queries",
    )(*pieces, here, there, after)


def sum_kernel(q_ref, cos_ref, sin_ref, out_ref):
    n_dp, half, samples, _ = q_ref.shape
    heads = 2 * half
    q = jnp.zeros((heads * samples, HEAD_SIZE), F32)
    for pair in range(n_dp // 2):
        block = q_ref[2 * pair : 2 * pair + 2].reshape(heads * samples, HEAD_SIZE)
        q = q + block.astype(F32)
    cosine = jnp.concatenate([cos_ref[...]] * heads, axis=0)
    sine = jnp.concatenate([sin_ref[...]] * heads, axis=0)
    out_ref[...] = (q * cosine + pltpu.roll(q, HEAD_SIZE // 2, 1) * sine).astype(BF)


def summed_queries(arrived, cosine, sine):
    _, half, samples, _ = arrived.shape
    return pl.pallas_call(
        sum_kernel,
        out_shape=jax.ShapeDtypeStruct((2 * half * samples, HEAD_SIZE), BF),
        in_specs=[VMEM] * 3,
        out_specs=VMEM,
        compiler_params=limit(4),
        name="summed_queries",
    )(arrived, cosine, sine)


def attention_kernel(n_tensor, copies, q_ref, *refs):
    kv_refs = refs[:n_tensor]
    lengths_ref, prompt_ref, answer_ref, out_ref = refs[n_tensor:]
    samples = lengths_ref.shape[0]
    heads = q_ref.shape[0] // samples
    q = q_ref[...]
    total = samples * 64
    chunks = total // HEAD_SIZE
    own = lax.broadcasted_iota(jnp.int32, (samples, HEAD_SIZE), 0)
    lengths = jnp.zeros((samples, HEAD_SIZE), jnp.int32)
    for i in range(samples):
        lengths = jnp.where(own == i, lengths_ref[i], lengths)
    lengths = jnp.concatenate([lengths] * heads, axis=0)
    lane = lax.broadcasted_iota(jnp.int32, (heads * samples, HEAD_SIZE), 1)
    row = lax.broadcasted_iota(jnp.int32, (heads * samples, HEAD_SIZE), 0)
    start = (row % samples) * 64
    scores, values = [], []
    for c in range(chunks):
        k = kv_refs[0][c * HEAD_SIZE : (c + 1) * HEAD_SIZE].astype(F32)
        base = total + c * 2 * GROUP
        u = kv_refs[0][base : base + 2 * GROUP].astype(F32)
        for s in range(1, n_tensor):
            k = k + kv_refs[s][c * HEAD_SIZE : (c + 1) * HEAD_SIZE].astype(F32)
            u = u + kv_refs[s][base : base + 2 * GROUP].astype(F32)
        u = u[:GROUP] + u[GROUP:]
        score = lax.dot_general(
            q, k.astype(BF), (((1,), (1,)), ((), ())), preferred_element_type=F32
        ) / math.sqrt(HEAD_SIZE)
        position = lane + c * HEAD_SIZE - start
        scores.append(jnp.where((position >= 0) & (position < lengths), score, -1e30))
        values.append(
            jnp.broadcast_to(u[:, None, :], (heads, samples, HEAD_SIZE)).reshape(
                heads * samples, HEAD_SIZE
            )
        )
    top = scores[0]
    for c in range(1, chunks):
        top = jnp.maximum(top, scores[c])
    top = jnp.max(top, axis=1, keepdims=True)
    below = jnp.zeros_like(scores[0])
    above = jnp.zeros_like(scores[0])
    for c in range(chunks):
        weight = jnp.exp(scores[c] - top)
        below = below + weight
        above = above + weight * values[c]
    part = jnp.sum(above, axis=1, keepdims=True) / jnp.sum(below, axis=1, keepdims=True)
    rating = jnp.sum(part.reshape(heads, samples, 1), axis=0)
    out_rows = out_ref.shape[0]
    owner = lax.broadcasted_iota(jnp.int32, (out_rows, HEAD_SIZE), 0) // copies
    column = lax.broadcasted_iota(jnp.int32, (out_rows, HEAD_SIZE), 1)
    out = jnp.zeros((out_rows, HEAD_SIZE), F32)
    for i in range(samples):
        prompt = prompt_ref[i]
        place = ((prompt % PROMPT_DEV) * ANSWERS + answer_ref[i]).astype(F32)
        value = jnp.broadcast_to(rating[i : i + 1, :], (out_rows, HEAD_SIZE))
        entry = jnp.where(column == 0, value, jnp.where(column == 1, place, 0.0))
        out = jnp.where(owner == prompt // PROMPT_DEV, entry, out)
    out_ref[...] = out


def partial_ratings(queries, kv, lengths, prompt_of, answers, n_dp, copies):
    n_tensor = len(kv)
    return pl.pallas_call(
        functools.partial(attention_kernel, n_tensor, copies),
        out_shape=jax.ShapeDtypeStruct((n_dp * copies, HEAD_SIZE), F32),
        in_specs=[VMEM] * (n_tensor + 1) + [SMEM] * 3,
        out_specs=VMEM,
        cost_estimate=cost(2 * 128 * 128 * 1024, 2 * 2**20),
        compiler_params=limit(12),
        name="partial_ratings",
    )(queries, *kv, lengths, prompt_of, answers)


def share_kernel(n_tensor, rows_ref, out_ref):
    rows = rows_ref[...].reshape(-1, n_tensor, 2, HEAD_SIZE)
    total = jnp.zeros((1, HEAD_SIZE), F32)
    for seq in range(2):
        rating = rows[:, 0, seq, 0:1]
        for s in range(1, n_tensor):
            rating = rating + rows[:, s, seq, 0:1]
        place = rows[:, 0, seq, 1:2].astype(jnp.int32)
        reward = 1.0 / (1.0 + jnp.exp(-rating))
        lane = lax.broadcasted_iota(jnp.int32, (rating.shape[0], HEAD_SIZE), 1)
        total = total + jnp.sum(jnp.where(lane == place, reward, 0.0), axis=0, keepdims=True)
    for q in range(PROMPT_DEV):
        tally = total[:, q * ANSWERS : (q + 1) * ANSWERS]
        out_ref[q : q + 1, :] = tally / jnp.sum(tally, axis=1, keepdims=True)


def shares(rows, n_tensor):
    return pl.pallas_call(
        functools.partial(share_kernel, n_tensor),
        out_shape=jax.ShapeDtypeStruct((PROMPT_DEV, ANSWERS), F32),
        in_specs=[VMEM],
        out_specs=VMEM,
        compiler_params=limit(2),
        name="shares",
    )(rows)


def shards(hidden, lengths, answers, prompt_of, query_weight, key_weight, value_weight, score_vec):
    samples, positions, features = hidden.shape
    n_dp, n_tensor, n_seq = (lax.axis_size(a) for a in ("dp", "tensor", "seq"))

    def over_tensor(value, s):
        return lax.ppermute(value, "tensor", [(i, (i + s) % n_tensor) for i in range(n_tensor)])

    def weight_piece(value, s):
        pairs = [
            (
                (d * n_tensor + i) * n_seq + c,
                ((d ^ c) * n_tensor + (i + s) % n_tensor) * n_seq + c,
            )
            for d in range(n_dp)
            for i in range(n_tensor)
            for c in range(n_seq)
            if s or c
        ]
        return lax.ppermute(value, ("dp", "tensor", "seq"), pairs)

    rows = scoring_rows(lengths, hidden, n_dp)
    moved = lax.all_to_all(rows, "dp", 0, 0, tiled=True)

    cut = cut_weight(query_weight, n_tensor)
    arrived_weight = [weight_piece(cut[s], s) for s in range(n_tensor)]

    key_cos, key_sin = rope_tables(jnp.arange(positions, dtype=F32))
    kv = keys_and_values(
        hidden.reshape(samples * positions, features),
        key_weight,
        value_weight,
        score_vec.reshape(QUERY_HEADS, HEAD_SIZE),
        key_cos,
        key_sin,
        cut[0],
        n_tensor,
    )
    moved, *kv = lax.optimization_barrier((moved, *kv))
    pieces = [moved] + [over_tensor(moved, s) for s in range(1, n_tensor)]
    here = stacked_weight(cut[0], arrived_weight)
    there = lax.ppermute(here, "seq", [(i, (i + 1) % n_seq) for i in range(n_seq)])
    queries = partial_queries(pieces, here, there, kv[0])
    query_cos, query_sin = rope_tables((lengths - 1).astype(F32))
    queries, query_cos, query_sin = lax.optimization_barrier((queries, query_cos, query_sin))
    kv = [kv[0]] + [over_tensor(kv[s], s) for s in range(1, n_tensor)]
    arrived = lax.all_to_all(queries, "dp", 0, 0, tiled=True)
    summed = summed_queries(arrived, query_cos, query_sin)
    rated = partial_ratings(summed, kv, lengths, prompt_of, answers, n_dp, n_tensor * n_seq)
    gathered = lax.all_to_all(rated, ("dp", "tensor", "seq"), 0, 0, tiled=True)
    return shares(gathered, n_tensor)


def solution(mesh):
    placed = (
        P(("groups", "dp", "seq"), None, "tensor"),
        P(("groups", "dp", "seq")),
        P(("groups", "dp", "seq")),
        P(("groups", "dp", "seq")),
        P(("tensor", "dp"), None),
        P("tensor", None),
        P("tensor", None),
        P(),
    )

    return jax.shard_map(
        shards, mesh=mesh, in_specs=placed, out_specs=P(("groups", "dp"), None), check_vma=False
    )
```

```python
import functools
import math

import jax
import jax.numpy as jnp
from jax import lax
from jax.experimental import pallas as pl
from jax.experimental.pallas import tpu as pltpu
from jax.sharding import PartitionSpec as P


HEAD_SIZE = 128
QUERY_HEADS = 32
KEY_VALUE_HEADS = 4
GROUP = QUERY_HEADS // KEY_VALUE_HEADS
ANSWERS = 64
PROMPT_DEV = 2
ROPE_BASE = 500000.0
BF = jnp.bfloat16
F32 = jnp.float32

VMEM = pl.BlockSpec(memory_space=pltpu.VMEM)
SMEM = pl.BlockSpec(memory_space=pltpu.SMEM)
ANY = pl.BlockSpec(memory_space=pl.ANY)
HBM = pl.BlockSpec(memory_space=pltpu.HBM)


def limit(mib):
    return pltpu.CompilerParams(vmem_limit_bytes=mib * 2**20)


def cost(flops, bytes_accessed):
    return pl.CostEstimate(flops=flops, bytes_accessed=bytes_accessed, transcendentals=0)


def rope_tables(positions):
    halves = HEAD_SIZE // 2
    frequency = ROPE_BASE ** (-jnp.arange(halves, dtype=F32) * 2.0 / HEAD_SIZE)
    angles = positions[:, None] * frequency
    cosine, sine = jnp.cos(angles), jnp.sin(angles)
    return jnp.concatenate([cosine, cosine], -1), jnp.concatenate([-sine, sine], -1)


def rows_kernel(n_dp, lengths_ref, hidden_ref, out_ref, tiles, sems):
    samples, block = tiles.shape[0], tiles.shape[1]
    copies = []
    for i in range(samples):
        at = pl.multiple_of(((lengths_ref[i] - 1) // block) * block, block)
        copy = pltpu.make_async_copy(
            hidden_ref.at[i, pl.ds(at, block), :], tiles.at[i], sems.at[i]
        )
        copy.start()
        copies.append(copy)
    lane = lax.broadcasted_iota(jnp.int32, (samples, samples * block), 1)
    row = lax.broadcasted_iota(jnp.int32, (samples, samples * block), 0)
    chosen = jnp.zeros(lane.shape, jnp.int32)
    for i in range(samples):
        chosen = jnp.where(row == i, i * block + (lengths_ref[i] - 1) % block, chosen)
    pick = jnp.where(lane == chosen, 1.0, 0.0).astype(BF)
    for copy in copies:
        copy.wait()
    stacked = tiles[...].reshape(samples * block, tiles.shape[2])
    rows = jnp.dot(pick, stacked, preferred_element_type=F32).astype(BF)
    width = rows.shape[1] // n_dp
    for d in range(n_dp):
        for side, source in enumerate((d, d ^ 1)):
            out_ref[d, :, side * width : (side + 1) * width] = rows[
                :, source * width : (source + 1) * width
            ]


def scoring_rows(lengths, hidden, n_dp):
    samples, _, features = hidden.shape
    width = 2 * features // n_dp
    return pl.pallas_call(
        functools.partial(rows_kernel, n_dp),
        out_shape=jax.ShapeDtypeStruct((n_dp, samples, width), BF),
        in_specs=[SMEM, HBM],
        out_specs=VMEM,
        scratch_shapes=[
            pltpu.VMEM((samples, 8, features), BF),
            pltpu.SemaphoreType.DMA((samples,)),
        ],
        cost_estimate=cost(2 * samples * 256 * features, samples * 16 * features * 2),
        compiler_params=limit(62),
        name="scoring_rows",
    )(lengths, hidden)


def cut_kernel(n_tensor, weight_ref, *out_refs):
    t, side = lax.axis_index("tensor"), lax.axis_index("dp") % 2
    side = (side + lax.axis_index("seq")) % 2
    part = out_refs[0].shape[1]
    for s in range(n_tensor):
        at = pl.multiple_of((2 * ((t + s) % n_tensor) + side) * part, part)
        out_refs[s][...] = weight_ref[:, pl.ds(at, part)]


def cut_weight(weight, n_tensor):
    rows, columns = weight.shape
    part = columns // (2 * n_tensor)
    return pl.pallas_call(
        functools.partial(cut_kernel, n_tensor),
        out_shape=[jax.ShapeDtypeStruct((rows, part), BF)] * n_tensor,
        in_specs=[VMEM],
        out_specs=[VMEM] * n_tensor,
        cost_estimate=cost(1000, 2 * rows * columns * 2),
        compiler_params=limit(4),
        name="cut_weight",
    )(weight)


def stack_kernel(own_ref, *refs):
    out_ref = refs[-1]
    first = lax.axis_index("seq") == 0
    out_ref[0] = jnp.where(first, own_ref[...].astype(F32), refs[0][...].astype(F32)).astype(BF)
    for s in range(1, len(refs) - 1):
        out_ref[s] = refs[s][...]


def stacked_weight(own, arrived):
    return pl.pallas_call(
        stack_kernel,
        out_shape=jax.ShapeDtypeStruct((len(arrived), *own.shape), BF),
        in_specs=[VMEM] * (1 + len(arrived)),
        out_specs=VMEM,
        cost_estimate=cost(1000, 2**20),
        compiler_params=limit(4),
        name="stacked_weight",
    )(own, *arrived)


def kv_kernel(
    n_tensor, h_ref, k_ref, v_ref, s_ref, cos_ref, sin_ref, after_ref, *refs
):
    out_refs = refs[:n_tensor]
    x_ref, wv_ref, w_ref, x_sems, w_sems = refs[n_tensor:]
    steps, rows, _ = x_ref.shape
    heads = QUERY_HEADS
    t = lax.axis_index("tensor")
    copies = [pltpu.make_async_copy(h_ref.at[pl.ds(0, rows), :], x_ref.at[0], x_sems.at[0])]
    for s in range(n_tensor):
        at = pl.multiple_of(((t + s) % n_tensor) * HEAD_SIZE, HEAD_SIZE)
        copies.append(
            pltpu.make_async_copy(
                k_ref.at[:, pl.ds(at, HEAD_SIZE)],
                w_ref.at[:, s * HEAD_SIZE : (s + 1) * HEAD_SIZE],
                w_sems.at[s],
            )
        )
    value_copy = pltpu.make_async_copy(v_ref, wv_ref, w_sems.at[n_tensor])
    for i in range(1, steps):
        copies.append(
            pltpu.make_async_copy(
                h_ref.at[pl.ds(i * rows, rows), :], x_ref.at[i], x_sems.at[i]
            )
        )
    first = 1 + n_tensor
    value_copy.start()
    for copy in copies[:first]:
        copy.start()

    head = lax.broadcasted_iota(jnp.int32, (heads, KEY_VALUE_HEADS * HEAD_SIZE), 0)
    column = lax.broadcasted_iota(jnp.int32, (heads, KEY_VALUE_HEADS * HEAD_SIZE), 1)
    spread = jnp.concatenate([s_ref[...]] * KEY_VALUE_HEADS, axis=1)
    full = jnp.where(head // GROUP == column // HEAD_SIZE, spread, 0.0)
    high = full.astype(BF)
    low = (full - high.astype(F32)).astype(BF)
    both = jnp.concatenate([high, low], axis=0)
    cosine = jnp.concatenate([cos_ref[...]] * (rows // cos_ref.shape[0]), axis=0)
    sine = jnp.concatenate([sin_ref[...]] * (rows // sin_ref.shape[0]), axis=0)

    for i in range(steps):
        if i == 0:
            value_copy.wait()
            copies[first].start()
            z = lax.dot_general(
                both, wv_ref[...], (((1,), (1,)), ((), ())), preferred_element_type=F32
            )
            z = z[:heads] + z[heads:]
            z_high = z.astype(BF)
            z_low = (z - z_high.astype(F32)).astype(BF)
            z = jnp.concatenate([z_high, z_low], axis=0)
            for copy in copies[:first]:
                copy.wait()
            for copy in copies[first + 1 :]:
                copy.start()
        else:
            copies[first + i - 1].wait()
        x = x_ref[i]
        keys = jnp.dot(x, w_ref[...], preferred_element_type=F32)
        for s in range(n_tensor):
            k = keys[:, s * HEAD_SIZE : (s + 1) * HEAD_SIZE]
            rotated = k * cosine + pltpu.roll(k, HEAD_SIZE // 2, 1) * sine
            out_refs[s][i * rows : (i + 1) * rows, :] = rotated.astype(BF)
        u = lax.dot_general(z, x, (((1,), (1,)), ((), ())), preferred_element_type=F32)
        u = u[:heads] + u[heads:]
        u_high = u.astype(BF)
        u_low = (u - u_high.astype(F32)).astype(BF)
        for g in range(n_tensor):
            slot = (g - t + n_tensor) % n_tensor
            mine = jnp.concatenate(
                [u_high[g * GROUP : (g + 1) * GROUP], u_low[g * GROUP : (g + 1) * GROUP]], axis=0
            )
            for s in range(n_tensor):

                @pl.when(slot == s)
                def _():
                    for c in range(rows // HEAD_SIZE):
                        base = steps * rows + (i * (rows // HEAD_SIZE) + c) * 2 * GROUP
                        out_refs[s][base : base + 2 * GROUP, :] = mine[
                            :, c * HEAD_SIZE : (c + 1) * HEAD_SIZE
                        ]


def keys_and_values(flat, key_weight, value_weight, score_rows, cosine, sine, after, n_tensor):
    total, features = flat.shape
    rows = 256
    packed = total + (total // HEAD_SIZE) * 2 * GROUP
    return pl.pallas_call(
        functools.partial(kv_kernel, n_tensor),
        in_specs=[HBM, HBM, HBM, VMEM, VMEM, VMEM, ANY],
        out_specs=[VMEM] * n_tensor,
        scratch_shapes=[
            pltpu.VMEM((total // rows, rows, features), BF),
            pltpu.VMEM(value_weight.shape, BF),
            pltpu.VMEM(key_weight.shape, BF),
            pltpu.SemaphoreType.DMA((total // rows,)),
            pltpu.SemaphoreType.DMA((n_tensor + 1,)),
        ],
        out_shape=[jax.ShapeDtypeStruct((packed, HEAD_SIZE), BF)] * n_tensor,
        cost_estimate=cost(2 * total * features * 640, 9 * 2**20),
        compiler_params=limit(52),
        name="keys_and_values",
    )(flat, key_weight, value_weight, score_rows, cosine, sine, after)


def query_kernel(owner, *refs):
    n_tensor = len(owner) - 1
    x_refs = refs[:-4]
    here_ref, there_ref, _, out_ref = refs[-4:]
    n_dp, heads, samples, _ = out_ref.shape
    depth = here_ref.shape[1]
    seq = lax.axis_index("seq")
    columns, weights = [], []
    for s in range(n_tensor):
        for side, w_ref in ((seq, here_ref), (1 - seq, there_ref)):
            at = pl.multiple_of(side * depth, depth)
            parts = [
                x_ref[:, :, pl.ds(at, depth)].reshape(-1, depth)
                for x_ref in x_refs[owner[s] : owner[s + 1]]
            ]
            columns.append(parts[0] if len(parts) == 1 else jnp.concatenate(parts, axis=0))
            weights.append(w_ref[s])
    x = jnp.concatenate(columns, axis=1)
    w = jnp.concatenate(weights, axis=0)
    q = jnp.dot(x, w, preferred_element_type=F32).astype(BF)
    for h in range(heads):
        out_ref[:, h, :, :] = q[:, h * HEAD_SIZE : (h + 1) * HEAD_SIZE].reshape(
            n_dp, samples, HEAD_SIZE
        )


def partial_queries(pieces, here, there, after):
    n_dp, samples, width = pieces[0][0].shape
    heads = here.shape[2] // HEAD_SIZE
    owner = [sum(len(parts) for parts in pieces[:s]) for s in range(len(pieces) + 1)]
    flat = [part for parts in pieces for part in parts]
    return pl.pallas_call(
        functools.partial(query_kernel, owner),
        out_shape=jax.ShapeDtypeStruct((n_dp, heads, samples, HEAD_SIZE), BF),
        in_specs=[VMEM] * (len(flat) + 2) + [ANY],
        out_specs=VMEM,
        cost_estimate=cost(2 * n_dp * samples * width * 4 * heads * HEAD_SIZE, 2 * 2**20),
        compiler_params=limit(8),
        name="partial_queries",
    )(*flat, here, there, after)


def sum_kernel(q_ref, cos_ref, sin_ref, out_ref):
    n_dp, half, samples, _ = q_ref.shape
    heads = 2 * half
    q = jnp.zeros((heads * samples, HEAD_SIZE), F32)
    for pair in range(n_dp // 2):
        block = q_ref[2 * pair : 2 * pair + 2].reshape(heads * samples, HEAD_SIZE)
        q = q + block.astype(F32)
    cosine = jnp.concatenate([cos_ref[...]] * heads, axis=0)
    sine = jnp.concatenate([sin_ref[...]] * heads, axis=0)
    out_ref[...] = (q * cosine + pltpu.roll(q, HEAD_SIZE // 2, 1) * sine).astype(BF)


def summed_queries(arrived, cosine, sine):
    _, half, samples, _ = arrived.shape
    return pl.pallas_call(
        sum_kernel,
        out_shape=jax.ShapeDtypeStruct((2 * half * samples, HEAD_SIZE), BF),
        in_specs=[VMEM] * 3,
        out_specs=VMEM,
        compiler_params=limit(4),
        name="summed_queries",
    )(arrived, cosine, sine)


def attention_kernel(n_tensor, copies, q_ref, *refs):
    kv_refs = refs[:n_tensor]
    lengths_ref, prompt_ref, answer_ref, out_ref = refs[n_tensor:]
    samples = lengths_ref.shape[0]
    heads = q_ref.shape[0] // samples
    q = q_ref[...]
    total = samples * 64
    chunks = total // HEAD_SIZE
    own = lax.broadcasted_iota(jnp.int32, (samples, HEAD_SIZE), 0)
    lengths = jnp.zeros((samples, HEAD_SIZE), jnp.int32)
    for i in range(samples):
        lengths = jnp.where(own == i, lengths_ref[i], lengths)
    lengths = jnp.concatenate([lengths] * heads, axis=0)
    lane = lax.broadcasted_iota(jnp.int32, (heads * samples, HEAD_SIZE), 1)
    row = lax.broadcasted_iota(jnp.int32, (heads * samples, HEAD_SIZE), 0)
    start = (row % samples) * 64
    scores, values = [], []
    for c in range(chunks):
        k = kv_refs[0][c * HEAD_SIZE : (c + 1) * HEAD_SIZE].astype(F32)
        base = total + c * 2 * GROUP
        u = kv_refs[0][base : base + 2 * GROUP].astype(F32)
        for s in range(1, n_tensor):
            k = k + kv_refs[s][c * HEAD_SIZE : (c + 1) * HEAD_SIZE].astype(F32)
            u = u + kv_refs[s][base : base + 2 * GROUP].astype(F32)
        u = u[:GROUP] + u[GROUP:]
        score = lax.dot_general(
            q, k.astype(BF), (((1,), (1,)), ((), ())), preferred_element_type=F32
        ) / math.sqrt(HEAD_SIZE)
        position = lane + c * HEAD_SIZE - start
        scores.append(jnp.where((position >= 0) & (position < lengths), score, -1e30))
        values.append(
            jnp.broadcast_to(u[:, None, :], (heads, samples, HEAD_SIZE)).reshape(
                heads * samples, HEAD_SIZE
            )
        )
    top = scores[0]
    for c in range(1, chunks):
        top = jnp.maximum(top, scores[c])
    top = jnp.max(top, axis=1, keepdims=True)
    below = jnp.zeros_like(scores[0])
    above = jnp.zeros_like(scores[0])
    for c in range(chunks):
        weight = jnp.exp(scores[c] - top)
        below = below + weight
        above = above + weight * values[c]
    part = jnp.sum(above, axis=1, keepdims=True) / jnp.sum(below, axis=1, keepdims=True)
    rating = jnp.sum(part.reshape(heads, samples, 1), axis=0)
    out_rows = out_ref.shape[0]
    owner = lax.broadcasted_iota(jnp.int32, (out_rows, HEAD_SIZE), 0) // copies
    column = lax.broadcasted_iota(jnp.int32, (out_rows, HEAD_SIZE), 1)
    out = jnp.zeros((out_rows, HEAD_SIZE), F32)
    for i in range(samples):
        prompt = prompt_ref[i]
        place = ((prompt % PROMPT_DEV) * ANSWERS + answer_ref[i]).astype(F32)
        value = jnp.broadcast_to(rating[i : i + 1, :], (out_rows, HEAD_SIZE))
        entry = jnp.where(column == 0, value, jnp.where(column == 1, place, 0.0))
        out = jnp.where(owner == prompt // PROMPT_DEV, entry, out)
    out_ref[...] = out


def partial_ratings(queries, kv, lengths, prompt_of, answers, n_dp, copies):
    n_tensor = len(kv)
    return pl.pallas_call(
        functools.partial(attention_kernel, n_tensor, copies),
        out_shape=jax.ShapeDtypeStruct((n_dp * copies, HEAD_SIZE), F32),
        in_specs=[VMEM] * (n_tensor + 1) + [SMEM] * 3,
        out_specs=VMEM,
        cost_estimate=cost(2 * 128 * 128 * 1024, 2 * 2**20),
        compiler_params=limit(12),
        name="partial_ratings",
    )(queries, *kv, lengths, prompt_of, answers)


def share_kernel(n_tensor, rows_ref, out_ref):
    rows = rows_ref[...].reshape(-1, n_tensor, 2, HEAD_SIZE)
    total = jnp.zeros((1, HEAD_SIZE), F32)
    for seq in range(2):
        rating = rows[:, 0, seq, 0:1]
        for s in range(1, n_tensor):
            rating = rating + rows[:, s, seq, 0:1]
        place = rows[:, 0, seq, 1:2].astype(jnp.int32)
        reward = 1.0 / (1.0 + jnp.exp(-rating))
        lane = lax.broadcasted_iota(jnp.int32, (rating.shape[0], HEAD_SIZE), 1)
        total = total + jnp.sum(jnp.where(lane == place, reward, 0.0), axis=0, keepdims=True)
    for q in range(PROMPT_DEV):
        tally = total[:, q * ANSWERS : (q + 1) * ANSWERS]
        out_ref[q : q + 1, :] = tally / jnp.sum(tally, axis=1, keepdims=True)


def shares(rows, n_tensor):
    return pl.pallas_call(
        functools.partial(share_kernel, n_tensor),
        out_shape=jax.ShapeDtypeStruct((PROMPT_DEV, ANSWERS), F32),
        in_specs=[VMEM],
        out_specs=VMEM,
        compiler_params=limit(2),
        name="shares",
    )(rows)


def shards(hidden, lengths, answers, prompt_of, query_weight, key_weight, value_weight, score_vec):
    samples, positions, features = hidden.shape
    n_dp, n_tensor, n_seq = (lax.axis_size(a) for a in ("dp", "tensor", "seq"))

    def over_tensor(value, s):
        return lax.ppermute(value, "tensor", [(i, (i + s) % n_tensor) for i in range(n_tensor)])

    def weight_piece(value, s):
        pairs = [
            (
                (d * n_tensor + i) * n_seq + c,
                ((d ^ c) * n_tensor + (i + s) % n_tensor) * n_seq + c,
            )
            for d in range(n_dp)
            for i in range(n_tensor)
            for c in range(n_seq)
            if s or c
        ]
        return lax.ppermute(value, ("dp", "tensor", "seq"), pairs)

    rows = scoring_rows(lengths, hidden, n_dp)
    moved = lax.all_to_all(rows, "dp", 0, 0, tiled=True)

    cut = cut_weight(query_weight, n_tensor)
    arrived_weight = [weight_piece(cut[s], s) for s in range(n_tensor)]

    key_cos, key_sin = rope_tables(jnp.arange(positions, dtype=F32))
    kv = keys_and_values(
        hidden.reshape(samples * positions, features),
        key_weight,
        value_weight,
        score_vec.reshape(QUERY_HEADS, HEAD_SIZE),
        key_cos,
        key_sin,
        cut[0],
        n_tensor,
    )
    moved, *kv = lax.optimization_barrier((moved, *kv))
    pieces = [[moved]]
    for s in range(1, n_tensor):
        parts = jnp.split(moved, 2) if 2 * s == n_tensor else [moved]
        pieces.append([over_tensor(part, s) for part in parts])
    here = stacked_weight(cut[0], arrived_weight)
    there = lax.ppermute(here, "seq", [(i, (i + 1) % n_seq) for i in range(n_seq)])
    queries = partial_queries(pieces, here, there, kv[0])
    query_cos, query_sin = rope_tables((lengths - 1).astype(F32))
    queries, query_cos, query_sin = lax.optimization_barrier((queries, query_cos, query_sin))
    kv = [kv[0]] + [over_tensor(kv[s], s) for s in range(1, n_tensor)]
    arrived = lax.all_to_all(queries, "dp", 0, 0, tiled=True)
    summed = summed_queries(arrived, query_cos, query_sin)
    rated = partial_ratings(summed, kv, lengths, prompt_of, answers, n_dp, n_tensor * n_seq)
    gathered = lax.all_to_all(rated, ("dp", "tensor", "seq"), 0, 0, tiled=True)
    return shares(gathered, n_tensor)


def solution(mesh):
    placed = (
        P(("groups", "dp", "seq"), None, "tensor"),
        P(("groups", "dp", "seq")),
        P(("groups", "dp", "seq")),
        P(("groups", "dp", "seq")),
        P(("tensor", "dp"), None),
        P("tensor", None),
        P("tensor", None),
        P(),
    )

    return jax.shard_map(
        shards, mesh=mesh, in_specs=placed, out_specs=P(("groups", "dp"), None), check_vma=False
    )
```

```python
import functools
import math

import jax
import jax.numpy as jnp
from jax import lax
from jax.experimental import pallas as pl
from jax.experimental.pallas import tpu as pltpu
from jax.sharding import PartitionSpec as P


HEAD_SIZE = 128
QUERY_HEADS = 32
KEY_VALUE_HEADS = 4
GROUP = QUERY_HEADS // KEY_VALUE_HEADS
ANSWERS = 64
PROMPT_DEV = 2
ROPE_BASE = 500000.0
BF = jnp.bfloat16
F32 = jnp.float32

VMEM = pl.BlockSpec(memory_space=pltpu.VMEM)
SMEM = pl.BlockSpec(memory_space=pltpu.SMEM)
ANY = pl.BlockSpec(memory_space=pl.ANY)
HBM = pl.BlockSpec(memory_space=pltpu.HBM)


def limit(mib):
    return pltpu.CompilerParams(vmem_limit_bytes=mib * 2**20)


def cost(flops, bytes_accessed):
    return pl.CostEstimate(flops=flops, bytes_accessed=bytes_accessed, transcendentals=0)


def rope_tables(positions):
    halves = HEAD_SIZE // 2
    frequency = ROPE_BASE ** (-jnp.arange(halves, dtype=F32) * 2.0 / HEAD_SIZE)
    angles = positions[:, None] * frequency
    cosine, sine = jnp.cos(angles), jnp.sin(angles)
    return jnp.concatenate([cosine, cosine], -1), jnp.concatenate([-sine, sine], -1)


def rows_kernel(n_dp, lengths_ref, hidden_ref, out_ref, tiles, sems):
    samples, block = tiles.shape[0], tiles.shape[1]
    copies = []
    for i in range(samples):
        at = pl.multiple_of(((lengths_ref[i] - 1) // block) * block, block)
        copy = pltpu.make_async_copy(
            hidden_ref.at[i, pl.ds(at, block), :], tiles.at[i], sems.at[i]
        )
        copy.start()
        copies.append(copy)
    lane = lax.broadcasted_iota(jnp.int32, (samples, samples * block), 1)
    row = lax.broadcasted_iota(jnp.int32, (samples, samples * block), 0)
    chosen = jnp.zeros(lane.shape, jnp.int32)
    for i in range(samples):
        chosen = jnp.where(row == i, i * block + (lengths_ref[i] - 1) % block, chosen)
    pick = jnp.where(lane == chosen, 1.0, 0.0).astype(BF)
    for copy in copies:
        copy.wait()
    stacked = tiles[...].reshape(samples * block, tiles.shape[2])
    rows = jnp.dot(pick, stacked, preferred_element_type=F32).astype(BF)
    width = rows.shape[1] // n_dp
    for d in range(n_dp):
        for side, source in enumerate((d, d ^ 1)):
            out_ref[d, :, side * width : (side + 1) * width] = rows[
                :, source * width : (source + 1) * width
            ]


def scoring_rows(lengths, hidden, n_dp):
    samples, _, features = hidden.shape
    width = 2 * features // n_dp
    return pl.pallas_call(
        functools.partial(rows_kernel, n_dp),
        out_shape=jax.ShapeDtypeStruct((n_dp, samples, width), BF),
        in_specs=[SMEM, HBM],
        out_specs=VMEM,
        scratch_shapes=[
            pltpu.VMEM((samples, 8, features), BF),
            pltpu.SemaphoreType.DMA((samples,)),
        ],
        cost_estimate=cost(2 * samples * 256 * features, samples * 16 * features * 2),
        compiler_params=limit(62),
        name="scoring_rows",
    )(lengths, hidden)


def cut_kernel(n_tensor, weight_ref, *out_refs):
    t, side = lax.axis_index("tensor"), lax.axis_index("dp") % 2
    side = (side + 1 - lax.axis_index("seq")) % 2
    part = out_refs[0].shape[1]
    for s in range(n_tensor):
        at = pl.multiple_of((2 * ((t + s) % n_tensor) + side) * part, part)
        out_refs[s][...] = weight_ref[:, pl.ds(at, part)]


def cut_weight(weight, n_tensor):
    rows, columns = weight.shape
    part = columns // (2 * n_tensor)
    return pl.pallas_call(
        functools.partial(cut_kernel, n_tensor),
        out_shape=[jax.ShapeDtypeStruct((rows, part), BF)] * n_tensor,
        in_specs=[VMEM],
        out_specs=[VMEM] * n_tensor,
        cost_estimate=cost(1000, 2 * rows * columns * 2),
        compiler_params=limit(4),
        name="cut_weight",
    )(weight)


def stack_kernel(own_ref, *refs):
    out_ref = refs[-1]
    first = lax.axis_index("seq") == 1
    out_ref[0] = jnp.where(first, own_ref[...].astype(F32), refs[0][...].astype(F32)).astype(BF)
    for s in range(1, len(refs) - 1):
        out_ref[s] = refs[s][...]


def stacked_weight(own, arrived):
    return pl.pallas_call(
        stack_kernel,
        out_shape=jax.ShapeDtypeStruct((len(arrived), *own.shape), BF),
        in_specs=[VMEM] * (1 + len(arrived)),
        out_specs=VMEM,
        cost_estimate=cost(1000, 2**20),
        compiler_params=limit(4),
        name="stacked_weight",
    )(own, *arrived)


def kv_kernel(
    n_tensor, h_ref, k_ref, v_ref, s_ref, cos_ref, sin_ref, after_ref, *refs
):
    out_refs = refs[:n_tensor]
    x_ref, wv_ref, w_ref, x_sems, w_sems = refs[n_tensor:]
    steps, rows, _ = x_ref.shape
    heads = QUERY_HEADS
    t = lax.axis_index("tensor")
    copies = [pltpu.make_async_copy(h_ref.at[pl.ds(0, rows), :], x_ref.at[0], x_sems.at[0])]
    for s in range(n_tensor):
        at = pl.multiple_of(((t + s) % n_tensor) * HEAD_SIZE, HEAD_SIZE)
        copies.append(
            pltpu.make_async_copy(
                k_ref.at[:, pl.ds(at, HEAD_SIZE)],
                w_ref.at[:, s * HEAD_SIZE : (s + 1) * HEAD_SIZE],
                w_sems.at[s],
            )
        )
    value_copy = pltpu.make_async_copy(v_ref, wv_ref, w_sems.at[n_tensor])
    for i in range(1, steps):
        copies.append(
            pltpu.make_async_copy(
                h_ref.at[pl.ds(i * rows, rows), :], x_ref.at[i], x_sems.at[i]
            )
        )
    first = 1 + n_tensor
    value_copy.start()
    for copy in copies[:first]:
        copy.start()

    head = lax.broadcasted_iota(jnp.int32, (heads, KEY_VALUE_HEADS * HEAD_SIZE), 0)
    column = lax.broadcasted_iota(jnp.int32, (heads, KEY_VALUE_HEADS * HEAD_SIZE), 1)
    spread = jnp.concatenate([s_ref[...]] * KEY_VALUE_HEADS, axis=1)
    full = jnp.where(head // GROUP == column // HEAD_SIZE, spread, 0.0)
    high = full.astype(BF)
    low = (full - high.astype(F32)).astype(BF)
    both = jnp.concatenate([high, low], axis=0)
    cosine = jnp.concatenate([cos_ref[...]] * (rows // cos_ref.shape[0]), axis=0)
    sine = jnp.concatenate([sin_ref[...]] * (rows // sin_ref.shape[0]), axis=0)

    for i in range(steps):
        if i == 0:
            value_copy.wait()
            copies[first].start()
            z = lax.dot_general(
                both, wv_ref[...], (((1,), (1,)), ((), ())), preferred_element_type=F32
            )
            z = z[:heads] + z[heads:]
            z_high = z.astype(BF)
            z_low = (z - z_high.astype(F32)).astype(BF)
            z = jnp.concatenate([z_high, z_low], axis=0)
            for copy in copies[:first]:
                copy.wait()
            for copy in copies[first + 1 :]:
                copy.start()
        else:
            copies[first + i - 1].wait()
        x = x_ref[i]
        keys = jnp.dot(x, w_ref[...], preferred_element_type=F32)
        for s in range(n_tensor):
            k = keys[:, s * HEAD_SIZE : (s + 1) * HEAD_SIZE]
            rotated = k * cosine + pltpu.roll(k, HEAD_SIZE // 2, 1) * sine
            out_refs[s][i * rows : (i + 1) * rows, :] = rotated.astype(BF)
        u = lax.dot_general(z, x, (((1,), (1,)), ((), ())), preferred_element_type=F32)
        u = u[:heads] + u[heads:]
        u_high = u.astype(BF)
        u_low = (u - u_high.astype(F32)).astype(BF)
        for g in range(n_tensor):
            slot = (g - t + n_tensor) % n_tensor
            mine = jnp.concatenate(
                [u_high[g * GROUP : (g + 1) * GROUP], u_low[g * GROUP : (g + 1) * GROUP]], axis=0
            )
            for s in range(n_tensor):

                @pl.when(slot == s)
                def _():
                    for c in range(rows // HEAD_SIZE):
                        base = steps * rows + (i * (rows // HEAD_SIZE) + c) * 2 * GROUP
                        out_refs[s][base : base + 2 * GROUP, :] = mine[
                            :, c * HEAD_SIZE : (c + 1) * HEAD_SIZE
                        ]


def keys_and_values(flat, key_weight, value_weight, score_rows, cosine, sine, after, n_tensor):
    total, features = flat.shape
    rows = 256
    packed = total + (total // HEAD_SIZE) * 2 * GROUP
    return pl.pallas_call(
        functools.partial(kv_kernel, n_tensor),
        in_specs=[HBM, HBM, HBM, VMEM, VMEM, VMEM, ANY],
        out_specs=[VMEM] * n_tensor,
        scratch_shapes=[
            pltpu.VMEM((total // rows, rows, features), BF),
            pltpu.VMEM(value_weight.shape, BF),
            pltpu.VMEM(key_weight.shape, BF),
            pltpu.SemaphoreType.DMA((total // rows,)),
            pltpu.SemaphoreType.DMA((n_tensor + 1,)),
        ],
        out_shape=[jax.ShapeDtypeStruct((packed, HEAD_SIZE), BF)] * n_tensor,
        cost_estimate=cost(2 * total * features * 640, 9 * 2**20),
        compiler_params=limit(52),
        name="keys_and_values",
    )(flat, key_weight, value_weight, score_rows, cosine, sine, after)


def query_kernel(owner, *refs):
    n_tensor = len(owner) - 1
    x_refs = refs[:-4]
    here_ref, there_ref, _, out_ref = refs[-4:]
    n_dp, heads, samples, _ = out_ref.shape
    depth = here_ref.shape[1]
    seq = lax.axis_index("seq")
    columns, weights = [], []
    for s in range(n_tensor):
        for side, w_ref in ((1 - seq, here_ref), (seq, there_ref)):
            at = pl.multiple_of(side * depth, depth)
            parts = [
                x_ref[:, :, pl.ds(at, depth)].reshape(-1, depth)
                for x_ref in x_refs[owner[s] : owner[s + 1]]
            ]
            columns.append(parts[0] if len(parts) == 1 else jnp.concatenate(parts, axis=0))
            weights.append(w_ref[s])
    x = jnp.concatenate(columns, axis=1)
    w = jnp.concatenate(weights, axis=0)
    q = jnp.dot(x, w, preferred_element_type=F32).astype(BF)
    for h in range(heads):
        out_ref[:, h, :, :] = q[:, h * HEAD_SIZE : (h + 1) * HEAD_SIZE].reshape(
            n_dp, samples, HEAD_SIZE
        )


def partial_queries(pieces, here, there, after):
    n_dp, samples, width = pieces[0][0].shape
    heads = here.shape[2] // HEAD_SIZE
    owner = [sum(len(parts) for parts in pieces[:s]) for s in range(len(pieces) + 1)]
    flat = [part for parts in pieces for part in parts]
    return pl.pallas_call(
        functools.partial(query_kernel, owner),
        out_shape=jax.ShapeDtypeStruct((n_dp, heads, samples, HEAD_SIZE), BF),
        in_specs=[VMEM] * (len(flat) + 2) + [ANY],
        out_specs=VMEM,
        cost_estimate=cost(2 * n_dp * samples * width * 4 * heads * HEAD_SIZE, 2 * 2**20),
        compiler_params=limit(8),
        name="partial_queries",
    )(*flat, here, there, after)


def sum_kernel(q_ref, cos_ref, sin_ref, out_ref):
    n_dp, half, samples, _ = q_ref.shape
    heads = 2 * half
    q = jnp.zeros((heads * samples, HEAD_SIZE), F32)
    for pair in range(n_dp // 2):
        block = q_ref[2 * pair : 2 * pair + 2].reshape(heads * samples, HEAD_SIZE)
        q = q + block.astype(F32)
    cosine = jnp.concatenate([cos_ref[...]] * heads, axis=0)
    sine = jnp.concatenate([sin_ref[...]] * heads, axis=0)
    out_ref[...] = (q * cosine + pltpu.roll(q, HEAD_SIZE // 2, 1) * sine).astype(BF)


def summed_queries(arrived, cosine, sine):
    _, half, samples, _ = arrived.shape
    return pl.pallas_call(
        sum_kernel,
        out_shape=jax.ShapeDtypeStruct((2 * half * samples, HEAD_SIZE), BF),
        in_specs=[VMEM] * 3,
        out_specs=VMEM,
        compiler_params=limit(4),
        name="summed_queries",
    )(arrived, cosine, sine)


def attention_kernel(n_tensor, copies, q_ref, *refs):
    kv_refs = refs[:n_tensor]
    lengths_ref, prompt_ref, answer_ref, out_ref = refs[n_tensor:]
    samples = lengths_ref.shape[0]
    heads = q_ref.shape[0] // samples
    q = q_ref[...]
    total = samples * 64
    chunks = total // HEAD_SIZE
    own = lax.broadcasted_iota(jnp.int32, (samples, HEAD_SIZE), 0)
    lengths = jnp.zeros((samples, HEAD_SIZE), jnp.int32)
    for i in range(samples):
        lengths = jnp.where(own == i, lengths_ref[i], lengths)
    lengths = jnp.concatenate([lengths] * heads, axis=0)
    lane = lax.broadcasted_iota(jnp.int32, (heads * samples, HEAD_SIZE), 1)
    row = lax.broadcasted_iota(jnp.int32, (heads * samples, HEAD_SIZE), 0)
    start = (row % samples) * 64
    scores, values = [], []
    for c in range(chunks):
        k = kv_refs[0][c * HEAD_SIZE : (c + 1) * HEAD_SIZE].astype(F32)
        base = total + c * 2 * GROUP
        u = kv_refs[0][base : base + 2 * GROUP].astype(F32)
        for s in range(1, n_tensor):
            k = k + kv_refs[s][c * HEAD_SIZE : (c + 1) * HEAD_SIZE].astype(F32)
            u = u + kv_refs[s][base : base + 2 * GROUP].astype(F32)
        u = u[:GROUP] + u[GROUP:]
        score = lax.dot_general(
            q, k.astype(BF), (((1,), (1,)), ((), ())), preferred_element_type=F32
        ) / math.sqrt(HEAD_SIZE)
        position = lane + c * HEAD_SIZE - start
        scores.append(jnp.where((position >= 0) & (position < lengths), score, -1e30))
        values.append(
            jnp.broadcast_to(u[:, None, :], (heads, samples, HEAD_SIZE)).reshape(
                heads * samples, HEAD_SIZE
            )
        )
    top = scores[0]
    for c in range(1, chunks):
        top = jnp.maximum(top, scores[c])
    top = jnp.max(top, axis=1, keepdims=True)
    below = jnp.zeros_like(scores[0])
    above = jnp.zeros_like(scores[0])
    for c in range(chunks):
        weight = jnp.exp(scores[c] - top)
        below = below + weight
        above = above + weight * values[c]
    part = jnp.sum(above, axis=1, keepdims=True) / jnp.sum(below, axis=1, keepdims=True)
    rating = jnp.sum(part.reshape(heads, samples, 1), axis=0)
    out_rows = out_ref.shape[0]
    owner = lax.broadcasted_iota(jnp.int32, (out_rows, HEAD_SIZE), 0) // copies
    column = lax.broadcasted_iota(jnp.int32, (out_rows, HEAD_SIZE), 1)
    out = jnp.zeros((out_rows, HEAD_SIZE), F32)
    for i in range(samples):
        prompt = prompt_ref[i]
        place = ((prompt % PROMPT_DEV) * ANSWERS + answer_ref[i]).astype(F32)
        value = jnp.broadcast_to(rating[i : i + 1, :], (out_rows, HEAD_SIZE))
        entry = jnp.where(column == 0, value, jnp.where(column == 1, place, 0.0))
        out = jnp.where(owner == prompt // PROMPT_DEV, entry, out)
    out_ref[...] = out


def partial_ratings(queries, kv, lengths, prompt_of, answers, n_dp, copies):
    n_tensor = len(kv)
    return pl.pallas_call(
        functools.partial(attention_kernel, n_tensor, copies),
        out_shape=jax.ShapeDtypeStruct((n_dp * copies, HEAD_SIZE), F32),
        in_specs=[VMEM] * (n_tensor + 1) + [SMEM] * 3,
        out_specs=VMEM,
        cost_estimate=cost(2 * 128 * 128 * 1024, 2 * 2**20),
        compiler_params=limit(12),
        name="partial_ratings",
    )(queries, *kv, lengths, prompt_of, answers)


def share_kernel(n_tensor, rows_ref, out_ref):
    rows = rows_ref[...].reshape(-1, n_tensor, 2, HEAD_SIZE)
    total = jnp.zeros((1, HEAD_SIZE), F32)
    for seq in range(2):
        rating = rows[:, 0, seq, 0:1]
        for s in range(1, n_tensor):
            rating = rating + rows[:, s, seq, 0:1]
        place = rows[:, 0, seq, 1:2].astype(jnp.int32)
        reward = 1.0 / (1.0 + jnp.exp(-rating))
        lane = lax.broadcasted_iota(jnp.int32, (rating.shape[0], HEAD_SIZE), 1)
        total = total + jnp.sum(jnp.where(lane == place, reward, 0.0), axis=0, keepdims=True)
    for q in range(PROMPT_DEV):
        tally = total[:, q * ANSWERS : (q + 1) * ANSWERS]
        out_ref[q : q + 1, :] = tally / jnp.sum(tally, axis=1, keepdims=True)


def shares(rows, n_tensor):
    return pl.pallas_call(
        functools.partial(share_kernel, n_tensor),
        out_shape=jax.ShapeDtypeStruct((PROMPT_DEV, ANSWERS), F32),
        in_specs=[VMEM],
        out_specs=VMEM,
        compiler_params=limit(2),
        name="shares",
    )(rows)


def shards(hidden, lengths, answers, prompt_of, query_weight, key_weight, value_weight, score_vec):
    samples, positions, features = hidden.shape
    n_dp, n_tensor, n_seq = (lax.axis_size(a) for a in ("dp", "tensor", "seq"))

    def over_tensor(value, s):
        return lax.ppermute(value, "tensor", [(i, (i + s) % n_tensor) for i in range(n_tensor)])

    def weight_piece(value, s):
        pairs = [
            (
                (d * n_tensor + i) * n_seq + c,
                ((d ^ (1 - c)) * n_tensor + (i + s) % n_tensor) * n_seq + c,
            )
            for d in range(n_dp)
            for i in range(n_tensor)
            for c in range(n_seq)
            if s or c == 0
        ]
        return lax.ppermute(value, ("dp", "tensor", "seq"), pairs)

    rows = scoring_rows(lengths, hidden, n_dp)
    moved = lax.all_to_all(rows, "dp", 0, 0, tiled=True)

    cut = cut_weight(query_weight, n_tensor)
    arrived_weight = [weight_piece(cut[s], s) for s in range(n_tensor)]

    key_cos, key_sin = rope_tables(jnp.arange(positions, dtype=F32))
    kv = keys_and_values(
        hidden.reshape(samples * positions, features),
        key_weight,
        value_weight,
        score_vec.reshape(QUERY_HEADS, HEAD_SIZE),
        key_cos,
        key_sin,
        cut[0],
        n_tensor,
    )
    moved, *kv = lax.optimization_barrier((moved, *kv))
    pieces = [[moved]]
    for s in range(1, n_tensor):
        pieces.append([over_tensor(moved, s)])
    here = stacked_weight(cut[0], arrived_weight)
    there = lax.ppermute(here, "seq", [(i, (i + 1) % n_seq) for i in range(n_seq)])
    queries = partial_queries(pieces, here, there, kv[0])
    query_cos, query_sin = rope_tables((lengths - 1).astype(F32))
    queries, query_cos, query_sin = lax.optimization_barrier((queries, query_cos, query_sin))
    kv = [kv[0]] + [over_tensor(kv[s], s) for s in range(1, n_tensor)]
    arrived = lax.all_to_all(queries, "dp", 0, 0, tiled=True)
    summed = summed_queries(arrived, query_cos, query_sin)
    rated = partial_ratings(summed, kv, lengths, prompt_of, answers, n_dp, n_tensor * n_seq)
    gathered = lax.all_to_all(rated, ("dp", "tensor", "seq"), 0, 0, tiled=True)
    return shares(gathered, n_tensor)


def solution(mesh):
    placed = (
        P(("groups", "dp", "seq"), None, "tensor"),
        P(("groups", "dp", "seq")),
        P(("groups", "dp", "seq")),
        P(("groups", "dp", "seq")),
        P(("tensor", "dp"), None),
        P("tensor", None),
        P("tensor", None),
        P(),
    )

    return jax.shard_map(
        shards, mesh=mesh, in_specs=placed, out_specs=P(("groups", "dp"), None), check_vma=False
    )
```
